128 devices in a mesh: rep: 1, r: 4 (over x), s: 32 (over y, z, core).
Axes of the slice: x: 4, y: 4, z: 4, core: 2. Of those that a mesh axis runs over, the one named last changes fastest.
Arguments:
- x: bfloat16 [128, 2048, 1024], P(('rep', 'r', 's'))
- dy: bfloat16 [128, 2048, 1024], P(('rep', 'r', 's'))
- w_gate: bfloat16 [2, 1024, 2560], P(None, 's')
- w_up: bfloat16 [2, 1024, 2560], P(None, 's')
- w_down: bfloat16 [2, 2560, 1024], P(None, 's')
Outputs:
- output 1: bfloat16 [128, 2048, 1024], P(('rep', 'r', 's'))
- output 2: bfloat16 [2, 1024, 2560], P('rep', 's')
- output 3: bfloat16 [2, 1024, 2560], P('rep', 's')
- output 4: bfloat16 [2, 2560, 1024], P('rep', 's')
All inputs are finite; a program needn't handle non-finite values.
Results may differ from the reference program's by a relative error of at most 0.018.
Values are sent between devices in bfloat16 or wider.
A program may use at most 1.5 GiB of HBM per device.

```python
import jax
import jax.numpy as jnp
from jax import lax

SEQUENCES = 128
TOKENS = 2048
D = 1024
FF = 2560
LAYERS = 2
NAMES = ("w_gate", "w_up", "w_down")
SHAPES = {"w_gate": (LAYERS, D, FF), "w_up": (LAYERS, D, FF), "w_down": (LAYERS, FF, D)}


def bump(key, n, height):
    away = (jnp.arange(n, dtype=jnp.int32) - jax.random.randint(key, (), 0, n, jnp.int32)) % n
    return jnp.where(away < n // 8, height, 1.0)


def together(key, own, strength):
    shared = jax.random.normal(key, own.shape[1:], jnp.float32)
    return (own + strength * shared) * lax.rsqrt(1 + strength * strength)


def setup_inputs(seed: int = 0, part: int = 0) -> dict:
    kx, kdy, ka, kb, kz, kf, kh, kl, *kw = jax.random.split(jax.random.key(seed), 8 + len(NAMES))
    kx, kdy, ka, kb = (jax.random.fold_in(k, part) for k in (kx, kdy, ka, kb))
    shape = (SEQUENCES, TOKENS, D)
    much_x, much_dy = jax.random.uniform(kz, (2,), jnp.float32, 0.0, 1.0)
    layers = 2.0 ** jax.random.uniform(kl, (LAYERS, 1, 1), jnp.float32, -1.0, 1.0)
    x = together(ka, jax.random.normal(kx, shape, jnp.float32), much_x) * bump(kf, D, 4.0)
    dy = together(kb, jax.random.normal(kdy, shape, jnp.float32), much_dy)
    drawn = {"x": x.astype(jnp.bfloat16), "dy": (dy * (SEQUENCES * TOKENS) ** -0.5).astype(jnp.bfloat16)}
    for key, name in zip(kw, NAMES, strict=True):
        w = jax.random.normal(key, SHAPES[name], jnp.float32) * SHAPES[name][1] ** -0.5
        drawn[name] = (w * {"w_gate": 1.0, "w_up": bump(kh, FF, 4.0), "w_down": layers}[name]).astype(jnp.bfloat16)
    return drawn


def matmul(a, w):
    return jnp.dot(a, w, preferred_element_type=jnp.float32).astype(jnp.bfloat16)


def normed(h):
    wide = h.astype(jnp.float32)
    scale = lax.rsqrt(jnp.mean(wide**2, -1, keepdims=True) + 1e-6)
    return (wide * scale).astype(jnp.bfloat16)


def layer(h, w):
    a = normed(h)
    gate = jnp.dot(a, w["w_gate"], preferred_element_type=jnp.float32)
    up = jnp.dot(a, w["w_up"], preferred_element_type=jnp.float32)
    return h + matmul((jax.nn.silu(gate) * up).astype(jnp.bfloat16), w["w_down"])


def stack(weights, h):
    return lax.scan(lambda h, w: (layer(h, w), None), h, weights)[0]


def reference(x, dy, w_gate, w_up, w_down):
    weights = dict(zip(NAMES, (w_gate, w_up, w_down), strict=True))

    def take(so_far, sequence):
        h, by_y = sequence
        _, back = jax.vjp(stack, weights, h)
        by_weights, by_h = back(by_y)
        return jax.tree.map(lambda total, term: total + term.astype(jnp.float32), so_far, by_weights), by_h

    none_yet = {name: jnp.zeros(w.shape, jnp.float32) for name, w in weights.items()}
    by_weights, by_x = lax.scan(take, none_yet, (x, dy))
    return (by_x, *(by_weights[name].astype(jnp.bfloat16) for name in NAMES))
```

```python
import functools

import jax
import jax.numpy as jnp
from jax import lax
from jax.experimental import pallas as pl
from jax.experimental.pallas import tpu as pltpu
from jax.sharding import PartitionSpec as P

F32, BF16 = jnp.float32, jnp.bfloat16
MESH = pl.DeviceIdType.MESH
ANY = pl.BlockSpec(memory_space=pl.ANY)
LIMIT = 60 * 1024 * 1024
SIZE = {"x": 4, "y": 4, "z": 4, "c": 2}


def here():
    s = lax.axis_index("s")
    return {"x": lax.axis_index("r"), "y": lax.div(s, 8), "z": lax.rem(lax.div(s, 2), 4), "c": lax.rem(s, 2)}


def moved(p, axis, step):
    return {**p, axis: lax.rem(p[axis] + step, SIZE[axis])}


def device(p):
    return {"r": p["x"], "s": (p["y"] * 4 + p["z"]) * 2 + p["c"]}


def greet(peers):
    me = here()
    barrier = pltpu.get_barrier_semaphore()
    for axis, step in peers:
        pl.semaphore_signal(barrier, inc=1, device_id=device(moved(me, axis, step)), device_id_type=MESH)
    pl.semaphore_wait(barrier, len(peers))


class Wires:
    def __init__(self, send, recv):
        self.send, self.recv, self.pending = send, recv, []

    def go(self, i, src, dst, to):
        copy = lambda: pltpu.make_async_remote_copy(src, dst, self.send.at[i], self.recv.at[i], device_id=device(to), device_id_type=MESH)
        copy().start()

    def sent(self, i, src, to):
        pltpu.make_async_remote_copy(src, src, self.send.at[i], self.recv.at[i], device_id=device(to), device_id_type=MESH).wait_send()

    def wait(self, i, dst, to):
        pltpu.make_async_remote_copy(dst, dst, self.send.at[i], self.recv.at[i], device_id=device(to), device_id_type=MESH).wait_recv()


GATHER_PEERS = (("c", 1), ("y", 1), ("y", 3), ("z", 1), ("z", 3))
GATHER_SEMS = 12


def gather_stages(first, second, w, full, local, send, recv):
    wires = Wires(send, recv)
    half = w.shape[-1] // 2
    left, right = pl.ds(0, half), pl.ds(half, half)

    def block(p, **free):
        p = {**p, **free}
        return full.at[p["y"], p["z"], p["c"]]

    def row(p, cols=None):
        p = {**p, first: slice(None)}
        return full.at[p["y"], p["z"], p["c"]] if cols is None else full.at[p["y"], p["z"], p["c"], :, cols]

    def part(p, cols):
        return full.at[p["y"], p["z"], p["c"], :, cols]

    def s0():
        me = here()
        pltpu.make_async_copy(w, block(me), local).start()
        wires.go(0, w, block(me), moved(me, first, 1))
        wires.go(1, w, block(me), moved(me, first, 3))

    def s1():
        me = here()
        before, after = moved(me, first, 3), moved(me, first, 1)
        wires.wait(0, block(before), before)
        wires.go(2, part(before, left), part(before, left), after)
        wires.wait(1, block(after), after)
        wires.go(3, part(after, right), part(after, right), before)
        pltpu.make_async_copy(w, block(me), local).wait()

    def s2():
        me = here()
        far = moved(me, first, 2)
        wires.wait(2, part(far, left), me)
        wires.wait(3, part(far, right), me)
        for i, (axis, step) in ((4, (second, 1)), (5, (second, 3)), (8, ("c", 1))):
            wires.go(i, row(me), row(me), moved(me, axis, step))

    def s3():
        me = here()
        before, after, mate = moved(me, second, 3), moved(me, second, 1), moved(me, "c", 1)
        wires.wait(4, row(before), before)
        wires.go(6, row(before, left), row(before, left), after)
        wires.wait(5, row(after), after)
        wires.go(7, row(after, right), row(after, right), before)
        wires.go(9, row(before), row(before), mate)
        wires.go(10, row(after), row(after), mate)

    def s4():
        me = here()
        far, mate = moved(me, second, 2), moved(me, "c", 1)
        wires.wait(6, row(far, left), me)
        wires.wait(7, row(far, right), me)
        wires.go(11, row(far), row(far), mate)

    def s5():
        me = here()
        mate = moved(me, "c", 1)
        for i, step in ((8, 0), (9, 3), (10, 1), (11, 2)):
            wires.wait(i, row(moved(mate, second, step)), me)
        for i in (0, 1):
            wires.sent(i, w, me)
        for i, cols in ((2, left), (3, right)):
            wires.sent(i, part(me, cols), me)
        for i in (4, 5, 8, 9, 10, 11):
            wires.sent(i, row(me), me)
        for i, cols in ((6, left), (7, right)):
            wires.sent(i, row(me, cols), me)

    return [s0, s1, s2, s3, s4, s5]


def gather_scratch(n):
    return [pltpu.SemaphoreType.DMA((n,)), pltpu.SemaphoreType.DMA((n, GATHER_SEMS)), pltpu.SemaphoreType.DMA((n, GATHER_SEMS))]


GATHER_ORDERS = (("z", "y"), ("y", "z"), ("z", "y"))


def gather_plan(ws, fulls, scratch):
    local, send, recv = scratch
    lists = [
        gather_stages(*GATHER_ORDERS[i % 3], w, full, local.at[i], send.at[i], recv.at[i])
        for i, (w, full) in enumerate(zip(ws, fulls, strict=True))
    ]
    return [[stages[k] for stages in lists] for k in range(len(lists[0]))]


def blocks_of(w):
    return (4, 4, 2, w.shape[0], w.shape[1])


def gather(ws, collective_id):
    n = len(ws)

    def kernel(*refs):
        plan = gather_plan(refs[:n], refs[n : 2 * n], refs[2 * n :])
        greet(GATHER_PEERS)
        for steps in plan:
            for step in steps:
                step()

    fulls = pl.pallas_call(
        kernel,
        out_shape=[jax.ShapeDtypeStruct(blocks_of(w), BF16) for w in ws],
        in_specs=[pl.BlockSpec(memory_space=pltpu.VMEM)] * n,
        out_specs=[ANY] * n,
        scratch_shapes=gather_scratch(n),
        compiler_params=pltpu.CompilerParams(collective_id=collective_id, has_side_effects=True),
        name="gather",
    )(*ws)
    return [f.reshape(-1, f.shape[-1]) for f in fulls]


SUM_PEERS = (("c", 1), *((axis, step) for axis in "xyz" for step in (1, 2, 3)))
SUM_SEMS = 18
SUM_ORDERS = ("xyz", "yzx", "zxy")


def sum_scratch(rows, columns):
    w = columns // 4
    vm = lambda *shape: pltpu.VMEM((*shape, rows, w), BF16)
    wide = lambda *shape: pltpu.VMEM((*shape, rows, w), F32)
    return [
        vm(4, 4, 4), vm(4, 4, 4),
        vm(2, 8), vm(2, 8), vm(2, 16), vm(2, 16), wide(16),
        vm(2, 2), vm(2, 2), vm(2, 4), vm(2, 4), wide(4),
        vm(3), vm(3), vm(4),
        pltpu.SemaphoreType.DMA((8,)), pltpu.SemaphoreType.DMA((SUM_SEMS,)), pltpu.SemaphoreType.DMA((SUM_SEMS,)),
    ]


SUM_REFS = 18


def sum_stages(order, term, out, refs):
    own, mates, o1, i1, o2, i2, k1, o3, i3, o4, i4, k2, o5, i5, ob, local, send, recv = refs
    wires = Wires(send, recv)
    A, B, D = order
    w = own.shape[-1]

    def at(**p):
        return p["y"], p["z"], p["x"]

    def chip(p):
        return own[at(**p)].astype(F32) + mates[at(**p)].astype(F32)

    def fetch(me, q):
        return pltpu.make_async_copy(term.at[:, :, me["c"], :, pl.ds(q * w, w)], own.at[:, :, q], local.at[q])

    def r0():
        me = here()
        mate = moved(me, "c", 1)
        for q in range(4):
            wires.go(q, term.at[:, :, mate["c"], :, pl.ds(q * w, w)], mates.at[:, :, q], mate)
            fetch(me, q).start()

    def r1():
        me = here()
        for q in range(4):
            fetch(me, q).wait()
            wires.wait(q, mates.at[:, :, q], me)
        far = lax.rem(me[A] + 2, 4)
        for turn, step in ((0, 1), (1, 3)):

            @pl.loop(0, 8)
            def _(i):
                b, d = lax.div(i, 4), lax.rem(i, 4)
                o1[turn, i] = chip({A: far, B: 2 * turn + b, D: d}).astype(BF16)

            wires.go(4 + turn, o1.at[turn], i1.at[turn], moved(me, A, step))

    def r2():
        me = here()
        for turn, step in ((0, 1), (1, 3)):
            wires.wait(4 + turn, i1.at[turn], me)
            to = moved(me, A, step)

            @pl.loop(0, 8)
            def _(i):
                b, d = lax.div(i, 4), lax.rem(i, 4)
                o2[turn, 8 * turn + i] = (chip({A: to[A], B: 2 * turn + b, D: d}) + i1[turn, i].astype(F32)).astype(BF16)
                o2[turn, 8 * (1 - turn) + i] = chip({A: to[A], B: 2 * (1 - turn) + b, D: d}).astype(BF16)

            wires.go(6 + turn, o2.at[turn], i2.at[turn], to)

    def r3():
        me = here()
        for turn in (0, 1):
            wires.wait(6 + turn, i2.at[turn], me)

        @pl.loop(0, 16)
        def _(i):
            k1[i] = chip({A: me[A], B: lax.div(i, 4), D: lax.rem(i, 4)}) + i2[0, i].astype(F32) + i2[1, i].astype(F32)

        far = lax.rem(me[B] + 2, 4)
        for turn, step in ((0, 1), (1, 3)):
            for d in range(2):
                o3[turn, d] = k1[far * 4 + 2 * turn + d].astype(BF16)
            wires.go(8 + turn, o3.at[turn], i3.at[turn], moved(me, B, step))

    def r4():
        me = here()
        for turn, step in ((0, 1), (1, 3)):
            wires.wait(8 + turn, i3.at[turn], me)
            to = moved(me, B, step)
            for d in range(2):
                o4[turn, 2 * turn + d] = (k1[to[B] * 4 + 2 * turn + d] + i3[turn, d].astype(F32)).astype(BF16)
                o4[turn, 2 * (1 - turn) + d] = k1[to[B] * 4 + 2 * (1 - turn) + d].astype(BF16)
            wires.go(10 + turn, o4.at[turn], i4.at[turn], to)

    def r5():
        me = here()
        for turn in (0, 1):
            wires.wait(10 + turn, i4.at[turn], me)
        for d in range(4):
            k2[d] = k1[me[B] * 4 + d] + i4[0, d].astype(F32) + i4[1, d].astype(F32)
        for j in (1, 2, 3):
            to = moved(me, D, j)
            o5[j - 1] = k2[to[D]].astype(BF16)
            wires.go(11 + j, o5.at[j - 1], i5.at[j - 1], to)

    def r6():
        me = here()
        total = k2[me[D]]
        for j in (1, 2, 3):
            wires.wait(11 + j, i5.at[j - 1], me)
            total = total + i5[j - 1].astype(F32)
        ob[me["x"]] = total.astype(BF16)
        for j in (1, 2, 3):
            wires.go(14 + j, ob.at[me["x"]], ob.at[me["x"]], moved(me, "x", j))

    def put(q):
        return pltpu.make_async_copy(ob.at[q], out.at[:, pl.ds(q * w, w)], local.at[4 + q])

    def r7():
        me = here()
        for j in (1, 2, 3):
            wires.wait(14 + j, ob.at[moved(me, "x", 4 - j)["x"]], me)
        for q in range(4):
            put(q).start()
        for q in range(4):
            wires.sent(q, mates.at[:, :, q], me)
        for turn in (0, 1):
            wires.sent(4 + turn, o1.at[turn], me)
            wires.sent(6 + turn, o2.at[turn], me)
            wires.sent(8 + turn, o3.at[turn], me)
            wires.sent(10 + turn, o4.at[turn], me)
        for j in (1, 2, 3):
            wires.sent(11 + j, o5.at[j - 1], me)
            wires.sent(14 + j, ob.at[me["x"]], me)
        for q in range(4):
            put(q).wait()

    return [r0, r1, r2, r3, r4, r5, r6, r7]


def sum_plan(terms, outs, scratch):
    lists = [sum_stages(SUM_ORDERS[i], terms[i], outs[i], scratch[SUM_REFS * i : SUM_REFS * (i + 1)]) for i in range(len(terms))]
    return [[stages[k] for stages in lists] for k in range(len(lists[0]))]


def cut(term):
    return term.reshape(4, 4, 2, term.shape[0] // 32, term.shape[1])


def summed(terms, collective_id):
    n = len(terms)
    terms = [cut(t) for t in terms]

    def kernel(*refs):
        plan = sum_plan(refs[:n], refs[n : 2 * n], refs[2 * n :])
        greet(SUM_PEERS)
        for steps in plan:
            for step in steps:
                step()

    return pl.pallas_call(
        kernel,
        out_shape=[jax.ShapeDtypeStruct(t.shape[3:], BF16) for t in terms],
        in_specs=[ANY] * n,
        out_specs=[ANY] * n,
        scratch_shapes=[s for t in terms for s in sum_scratch(*t.shape[3:])],
        compiler_params=pltpu.CompilerParams(collective_id=collective_id, has_side_effects=True, vmem_limit_bytes=LIMIT),
        name="summed",
    )(*terms)


def dot(a, b, dims=((1,), (0,))):
    return lax.dot_general(a, b, (dims, ((), ())), preferred_element_type=F32)


def scale_of(wide):
    return lax.rsqrt(jnp.mean(wide * wide, -1, keepdims=True) + 1e-6)


def norm_into(h, a, at, chunk=512):
    @pl.loop(0, h.shape[0], step=chunk)
    def _(m):
        rows = pl.ds(m, chunk)
        wide = h[rows, :].astype(F32)
        value = (wide * scale_of(wide)).astype(BF16)
        if a is not None:
            a[rows, :] = value
        if at is not None:
            at[:, rows] = value.T


def whole(shape):
    return pl.BlockSpec(shape, lambda i: (0,) * len(shape), pipeline_mode=pl.Buffered(1))


TILE, CHUNK = 256, 512


def forward(h, wg, wu, wd):
    tokens, d = h.shape
    ff = wg.shape[1]
    steps = ff // TILE

    def kernel(h_ref, wg_ref, wu_ref, wd_ref, y_ref, g_ref, u_ref, at_ref, a, acc):
        i = pl.program_id(0)

        @pl.when(i == 0)
        def _():
            norm_into(h_ref, a, at_ref)
            acc[...] = jnp.zeros_like(acc)

        @pl.loop(0, tokens, step=CHUNK)
        def _(m):
            rows = pl.ds(m, CHUNK)
            g = dot(a[rows, :], wg_ref[...])
            u = dot(a[rows, :], wu_ref[...])
            g_ref[rows, :] = g
            u_ref[rows, :] = u
            act = (g * jax.nn.sigmoid(g) * u).astype(BF16)
            acc[rows, :] += dot(act, wd_ref[...])

        @pl.when(i == steps - 1)
        def _():
            y_ref[...] = h_ref[...] + acc[...].astype(BF16)

    across = pl.BlockSpec((d, TILE), lambda i: (0, i))
    tile = pl.BlockSpec((tokens, TILE), lambda i: (0, i))
    return pl.pallas_call(
        kernel,
        grid=(steps,),
        out_shape=[
            jax.ShapeDtypeStruct(h.shape, BF16),
            jax.ShapeDtypeStruct((tokens, ff), F32),
            jax.ShapeDtypeStruct((tokens, ff), F32),
            jax.ShapeDtypeStruct((d, tokens), BF16),
        ],
        in_specs=[whole(h.shape), across, across, pl.BlockSpec((TILE, d), lambda i: (i, 0))],
        out_specs=[whole(h.shape), tile, tile, whole((d, tokens))],
        scratch_shapes=[pltpu.VMEM(h.shape, BF16), pltpu.VMEM(h.shape, F32)],
        compiler_params=pltpu.CompilerParams(vmem_limit_bytes=LIMIT),
        name="forward",
    )(h, wg, wu, wd)


def hidden_grads(g, u, by_act):
    sig = jax.nn.sigmoid(g)
    silu = g * sig
    by_act = by_act.astype(BF16).astype(F32)
    return (silu * u).astype(BF16), (by_act * u * (sig * (1 + g * (1 - sig)))).astype(BF16), (by_act * silu).astype(BF16)


def backward_hidden(by_y, wd, saved=None, fresh=None):
    tokens, d = by_y.shape
    ff = wd.shape[0]
    steps = ff // TILE

    def kernel(*refs):
        i = pl.program_id(0)
        if fresh is not None:
            h_ref, wg_ref, wu_ref, by_ref, wd_ref, dg_ref, du_ref, dwg_ref, dwu_ref, dwd_ref, act, a, at = refs

            @pl.when(i == 0)
            def _():
                norm_into(h_ref, a, at)
        else:
            at, g_ref, u_ref, by_ref, wd_ref, dg_ref, du_ref, dwg_ref, dwu_ref, dwd_ref, act = refs

        @pl.loop(0, tokens, step=CHUNK)
        def _(m):
            rows = pl.ds(m, CHUNK)
            if fresh is not None:
                g, u = dot(a[rows, :], wg_ref[...]), dot(a[rows, :], wu_ref[...])
            else:
                g, u = g_ref[rows, :], u_ref[rows, :]
            by_act = dot(by_ref[rows, :], wd_ref[...], ((1,), (1,)))
            act[rows, :], dg_ref[rows, :], du_ref[rows, :] = hidden_grads(g, u, by_act)

        dwd_ref[...] = dot(act[...], by_ref[...], ((0,), (0,))).astype(BF16)
        dwg_ref[...] = dot(at[...], dg_ref[...]).astype(BF16)
        dwu_ref[...] = dot(at[...], du_ref[...]).astype(BF16)

    across = pl.BlockSpec((d, TILE), lambda i: (0, i))
    down = pl.BlockSpec((TILE, d), lambda i: (i, 0))
    tile = pl.BlockSpec((tokens, TILE), lambda i: (0, i))
    scratch = [pltpu.VMEM((tokens, TILE), BF16)]
    if fresh is not None:
        specs = [whole((tokens, d)), across, across]
        scratch += [pltpu.VMEM((tokens, d), BF16), pltpu.VMEM((d, tokens), BF16)]
    else:
        specs = [whole((d, tokens)), tile, tile]
    return pl.pallas_call(
        kernel,
        grid=(steps,),
        out_shape=[jax.ShapeDtypeStruct((tokens, ff), BF16)] * 2 + [jax.ShapeDtypeStruct((d, ff), BF16)] * 2 + [jax.ShapeDtypeStruct((ff, d), BF16)],
        in_specs=specs + [whole((tokens, d)), down],
        out_specs=[tile, tile, across, across, down],
        scratch_shapes=scratch,
        compiler_params=pltpu.CompilerParams(vmem_limit_bytes=LIMIT),
        name="backward_hidden",
    )(*(fresh if fresh is not None else saved), by_y, wd)


def backward_input(dg, du, wg, wu, h, by_y):
    tokens, d = h.shape
    ff = dg.shape[1]
    chunk = 256

    def kernel(dg_ref, du_ref, wg_ref, wu_ref, h_ref, by_ref, out_ref):
        by_a = dot(dg_ref[...], wg_ref[...], ((1,), (1,))) + dot(du_ref[...], wu_ref[...], ((1,), (1,)))
        by_a = by_a.astype(BF16).astype(F32)
        wide = h_ref[...].astype(F32)
        scale = scale_of(wide)
        back = jnp.sum(by_a * wide, -1, keepdims=True) * (scale * scale * scale) * (1 / d)
        out_ref[...] = by_ref[...] + (by_a * scale - wide * back).astype(BF16)

    rows = lambda n: pl.BlockSpec((chunk, n), lambda i: (i, 0))
    return pl.pallas_call(
        kernel,
        grid=(tokens // chunk,),
        out_shape=jax.ShapeDtypeStruct(h.shape, BF16),
        in_specs=[rows(ff), rows(ff), whole(wg.shape), whole(wu.shape), rows(d), rows(d)],
        out_specs=rows(d),
        compiler_params=pltpu.CompilerParams(vmem_limit_bytes=LIMIT),
        name="backward_input",
    )(dg, du, wg, wu, h, by_y)


def solution(mesh):
    def step(x, dy, *weights):
        x, dy = x[0], dy[0]
        w0 = gather([w[0] for w in weights], 1)
        w1 = gather([w[1] for w in weights], 1)
        h1, g0, u0, at0 = forward(x, *w0)
        dg1, du1, *terms1 = backward_hidden(dy, w1[2], fresh=(h1, w1[0], w1[1]))
        by_h1 = backward_input(dg1, du1, w1[0], w1[1], h1, dy)
        dg0, du0, *terms0 = backward_hidden(by_h1, w0[2], saved=(at0, g0, u0))
        by_x = backward_input(dg0, du0, w0[0], w0[1], x, by_h1)
        sums1 = summed(terms1, 2)
        sums0 = summed(terms0, 2)
        return (by_x[None], *(jnp.stack([sums0[i], sums1[i]]) for i in range(3)))

    states, shard = P(("rep", "r", "s"), None, None), P(None, "s", None)
    return jax.shard_map(
        step,
        mesh=mesh,
        in_specs=(states, states) + (shard,) * 3,
        out_specs=(states,) + (P("rep", "s", None),) * 3,
        check_vma=False,
    )
```

```python
import functools

import jax
import jax.numpy as jnp
from jax import lax
from jax.experimental import pallas as pl
from jax.experimental.pallas import tpu as pltpu
from jax.sharding import PartitionSpec as P

F32, BF16 = jnp.float32, jnp.bfloat16
MESH = pl.DeviceIdType.MESH
ANY = pl.BlockSpec(memory_space=pl.ANY)
LIMIT = 66_000_000
SIZE = {"x": 4, "y": 4, "z": 4, "c": 2}


def here():
    s = lax.axis_index("s")
    return {"x": lax.axis_index("r"), "y": lax.div(s, 8), "z": lax.rem(lax.div(s, 2), 4), "c": lax.rem(s, 2)}


def moved(p, axis, step):
    return {**p, axis: lax.rem(p[axis] + step, SIZE[axis])}


def device(p):
    return {"r": p["x"], "s": (p["y"] * 4 + p["z"]) * 2 + p["c"]}


def greet(peers):
    me = here()
    barrier = pltpu.get_barrier_semaphore()
    for peer in peers:
        to = me
        for axis, step in peer if isinstance(peer[0], tuple) else (peer,):
            to = moved(to, axis, step)
        pl.semaphore_signal(barrier, inc=1, device_id=device(to), device_id_type=MESH)
    pl.semaphore_wait(barrier, len(peers))


class Wires:
    def __init__(self, send, recv):
        self.send, self.recv, self.pending = send, recv, []

    def go(self, i, src, dst, to):
        copy = lambda: pltpu.make_async_remote_copy(src, dst, self.send.at[i], self.recv.at[i], device_id=device(to), device_id_type=MESH)
        copy().start()

    def sent(self, i, src, to):
        pltpu.make_async_remote_copy(src, src, self.send.at[i], self.recv.at[i], device_id=device(to), device_id_type=MESH).wait_send()

    def wait(self, i, dst, to):
        pltpu.make_async_remote_copy(dst, dst, self.send.at[i], self.recv.at[i], device_id=device(to), device_id_type=MESH).wait_recv()


def gather_stages(first, second, w, full, local, send, recv):
    wires = Wires(send, recv)
    half = w.shape[-1] // 2
    left, right = pl.ds(0, half), pl.ds(half, half)

    def block(p, **free):
        p = {**p, **free}
        return full.at[p["y"], p["z"], p["c"]]

    def row(p, cols=None):
        p = {**p, first: slice(None)}
        return full.at[p["y"], p["z"], p["c"]] if cols is None else full.at[p["y"], p["z"], p["c"], :, cols]

    def part(p, cols):
        return full.at[p["y"], p["z"], p["c"], :, cols]

    def s0():
        me = here()
        pltpu.make_async_copy(w, block(me), local).start()
        wires.go(0, w, block(me), moved(me, first, 1))
        wires.go(1, w, block(me), moved(me, first, 3))

    def s1():
        me = here()
        before, after = moved(me, first, 3), moved(me, first, 1)
        wires.wait(0, block(before), before)
        wires.go(2, part(before, left), part(before, left), after)
        wires.wait(1, block(after), after)
        wires.go(3, part(after, right), part(after, right), before)
        pltpu.make_async_copy(w, block(me), local).wait()

    def s2():
        me = here()
        far = moved(me, first, 2)
        wires.wait(2, part(far, left), me)
        wires.wait(3, part(far, right), me)
        for i, (axis, step) in ((4, (second, 1)), (5, (second, 3)), (8, ("c", 1))):
            wires.go(i, row(me), row(me), moved(me, axis, step))

    def s3():
        me = here()
        before, after, mate = moved(me, second, 3), moved(me, second, 1), moved(me, "c", 1)
        wires.wait(4, row(before), before)
        wires.go(6, row(before, left), row(before, left), after)
        wires.wait(5, row(after), after)
        wires.go(7, row(after, right), row(after, right), before)
        wires.go(9, row(before), row(before), mate)
        wires.go(10, row(after), row(after), mate)

    def s4():
        me = here()
        far, mate = moved(me, second, 2), moved(me, "c", 1)
        wires.wait(6, row(far, left), me)
        wires.wait(7, row(far, right), me)
        wires.go(11, row(far), row(far), mate)

    def s5():
        me = here()
        mate = moved(me, "c", 1)
        for i, step in ((8, 0), (9, 3), (10, 1), (11, 2)):
            wires.wait(i, row(moved(mate, second, step)), me)
        for i in (0, 1):
            wires.sent(i, w, me)
        for i, cols in ((2, left), (3, right)):
            wires.sent(i, part(me, cols), me)
        for i in (4, 5, 8, 9, 10, 11):
            wires.sent(i, row(me), me)
        for i, cols in ((6, left), (7, right)):
            wires.sent(i, row(me, cols), me)

    return [s0, s1, s2, s3, s4, s5]


def gather_stages_x(first, second, w, full, local, send, recv):
    wires = Wires(send, recv)
    quarter = w.shape[-1] // 4
    half = quarter // 2

    def cols(q, at=0, size=quarter):
        return pl.ds(pl.multiple_of(q * quarter + at, half), size)

    def part(p, c, **free):
        p = {**p, **free}
        return full.at[p["y"], p["z"], p["c"], :, c]

    def row(p, c):
        return part(p, c, **{first: slice(None)})

    def plane(p, q, ys=slice(None)):
        return full.at[ys, :, p["c"], :, cols(q)]

    def halves(me):
        return cols(me["x"], 0, half), cols(me["x"], half, half)

    def s0():
        me = here()
        q = cols(me["x"])
        pltpu.make_async_copy(w.at[:, q], part(me, q), local).start()
        wires.go(0, w.at[:, q], part(me, q), moved(me, first, 1))
        wires.go(1, w.at[:, q], part(me, q), moved(me, first, 3))

    def s1():
        me = here()
        q, (left, right) = cols(me["x"]), halves(me)
        before, after = moved(me, first, 3), moved(me, first, 1)
        wires.wait(0, part(before, q), before)
        wires.go(2, part(before, left), part(before, left), after)
        wires.wait(1, part(after, q), after)
        wires.go(3, part(after, right), part(after, right), before)
        pltpu.make_async_copy(w.at[:, q], part(me, q), local).wait()

    def s2():
        me = here()
        q, (left, right) = cols(me["x"]), halves(me)
        far = moved(me, first, 2)
        wires.wait(2, part(far, left), me)
        wires.wait(3, part(far, right), me)
        wires.go(4, row(me, q), row(me, q), moved(me, second, 1))
        wires.go(5, row(me, q), row(me, q), moved(me, second, 3))

    def s3():
        me = here()
        q, (left, right) = cols(me["x"]), halves(me)
        before, after = moved(me, second, 3), moved(me, second, 1)
        wires.wait(4, row(before, q), before)
        wires.go(6, row(before, left), row(before, left), after)
        wires.wait(5, row(after, q), after)
        wires.go(7, row(after, right), row(after, right), before)

    def s4():
        me = here()
        left, right = halves(me)
        far = moved(me, second, 2)
        wires.wait(6, row(far, left), me)
        wires.wait(7, row(far, right), me)
        q = me["x"]
        for i, (axis, step) in ((8, ("x", 1)), (9, ("x", 3)), (12, ("c", 1))):
            wires.go(i, plane(me, q), plane(me, q), moved(me, axis, step))

    low, high = slice(0, 2), slice(2, 4)

    def s5():
        me = here()
        before, after, mate = moved(me, "x", 3), moved(me, "x", 1), moved(me, "c", 1)
        wires.wait(8, plane(me, before["x"]), me)
        wires.go(10, plane(me, before["x"], low), plane(me, before["x"], low), after)
        wires.wait(9, plane(me, after["x"]), me)
        wires.go(11, plane(me, after["x"], high), plane(me, after["x"], high), before)
        wires.go(13, plane(me, before["x"]), plane(me, before["x"]), mate)
        wires.go(14, plane(me, after["x"]), plane(me, after["x"]), mate)

    def s6():
        me = here()
        far, mate = moved(me, "x", 2)["x"], moved(me, "c", 1)
        wires.wait(10, plane(me, far, low), me)
        wires.wait(11, plane(me, far, high), me)
        wires.go(15, plane(me, far), plane(me, far), mate)

    def s7():
        me = here()
        mate = moved(me, "c", 1)
        q, (left, right) = cols(me["x"]), halves(me)
        for i, step in ((12, 0), (13, 3), (14, 1), (15, 2)):
            wires.wait(i, plane(mate, moved(me, "x", step)["x"]), me)
        for i in (0, 1):
            wires.sent(i, w.at[:, q], me)
        for i, c in ((2, left), (3, right)):
            wires.sent(i, part(me, c), me)
        for i, c in ((4, q), (5, q), (6, left), (7, right)):
            wires.sent(i, row(me, c), me)
        for i in (8, 9, 12, 13, 14, 15):
            wires.sent(i, plane(me, me["x"]), me)
        for i, ys in ((10, low), (11, high)):
            wires.sent(i, plane(me, me["x"], ys), me)

    return [s0, s1, s2, s3, s4, s5, s6, s7]


def gather_stages_direct(w, full, local, send, recv, start, size):
    wires = Wires(send, recv)
    cols = pl.ds(start, size)
    others = [(j, k) for j in (1, 3, 0, 2) for k in (1, 3, 0, 2) if (j, k) != (0, 0)]

    def part(p):
        return full.at[p["y"], p["z"], p["c"], :, cols]

    def every(c):
        return full.at[:, :, c, :, cols]

    def s0():
        me = here()
        for n, (j, k) in enumerate(others):
            wires.go(n, w.at[:, cols], part(me), moved(moved(me, "y", j), "z", k))
        pltpu.make_async_copy(w.at[:, cols], part(me), local).start()

    def s1():
        me = here()
        pltpu.make_async_copy(w.at[:, cols], part(me), local).wait()
        for n, (j, k) in enumerate(others):
            wires.wait(n, part(moved(moved(me, "y", 4 - j), "z", 4 - k)), me)
        wires.go(15, every(me["c"]), every(me["c"]), moved(me, "c", 1))

    def s2():
        wires.wait(15, every(moved(here(), "c", 1)["c"]), here())

    def s3():
        me = here()
        for n in range(15):
            wires.sent(n, w.at[:, cols], me)
        wires.sent(15, every(me["c"]), me)

    return [s0, s1, s2, s3]


def blocks_of(w):
    return (4, 4, 2, w.shape[0], w.shape[1])


PLANE_PEERS = (("c", 1), ("x", 1), ("x", 3), *((("y", j), ("z", k)) for j in range(4) for k in range(4) if j or k))


class Exchange:
    def before(self):
        greet(self.peers)

    def grid_step(self, plan, marks, i):
        for at, steps in marks.items():
            if at != "end":

                @pl.when(i == at)
                def _():
                    if at == 0:
                        self.before()
                    for which, number in steps:
                        plan[which][number]()

    def finish(self, plan, marks):
        for which, number in marks["end"]:
            plan[which][number]()


class Gather(Exchange):
    peers = (("c", 1), *((axis, step) for axis in "yz" for step in (1, 2, 3)), ("x", 1), ("x", 3))

    def __init__(self, ws):
        n = len(ws)
        self.operands = list(ws)
        self.in_specs = [pl.BlockSpec(memory_space=pltpu.VMEM)] * n
        self.out_shape = [jax.ShapeDtypeStruct(blocks_of(w), BF16) for w in ws]
        self.out_specs = [ANY] * n
        sems = [12, 12, 16]
        self.scratch = [pltpu.SemaphoreType.DMA((n,))] + [pltpu.SemaphoreType.DMA((k,)) for k in sems for _ in range(2)]

    def plan(self, ins, outs, scratch):
        local, *sems = scratch
        makers = (functools.partial(gather_stages, "z", "y"), functools.partial(gather_stages, "y", "z"), functools.partial(gather_stages_x, "z", "y"))
        return [make(w, full, local.at[i], sems[2 * i], sems[2 * i + 1]) for i, (make, w, full) in enumerate(zip(makers, ins, outs, strict=True))]

    @staticmethod
    def whole_matrices(fulls):
        return [f.reshape(-1, f.shape[-1]) for f in fulls]


def gather_stages_chunk(first, second, w, full, local, send, recv, start, size, to=None):
    wires = Wires(send, recv)
    to = start if to is None else to
    source = w.at[:, pl.ds(start, size)]
    cols, left, right = pl.ds(to, size), pl.ds(to, size // 2), pl.ds(to + size // 2, size // 2)

    def part(p, c):
        return full.at[p["y"], p["z"], p["c"], :, c]

    def row(p, c):
        return part({**p, first: slice(None)}, c)

    def s0():
        me = here()
        for j in (1, 3, 2):
            wires.go(j - 1, source, part(me, cols), moved(me, first, j))
        pltpu.make_async_copy(source, part(me, cols), local).start()

    def s1():
        me = here()
        pltpu.make_async_copy(source, part(me, cols), local).wait()
        for j in (1, 3, 2):
            wires.wait(j - 1, part(moved(me, first, 4 - j), cols), me)
        wires.go(3, row(me, cols), row(me, cols), moved(me, second, 1))
        wires.go(4, row(me, cols), row(me, cols), moved(me, second, 3))

    def s2():
        me = here()
        before, after = moved(me, second, 3), moved(me, second, 1)
        wires.wait(3, row(before, cols), me)
        wires.go(5, row(before, left), row(before, left), after)
        wires.wait(4, row(after, cols), me)
        wires.go(6, row(after, right), row(after, right), before)

    def every(c):
        return full.at[:, :, c, :, cols]

    def s3():
        me = here()
        far, mate = moved(me, second, 2), moved(me, "c", 1)
        wires.wait(5, row(far, left), me)
        wires.wait(6, row(far, right), me)
        wires.go(7, every(me["c"]), every(me["c"]), mate)

    def s4():
        me = here()
        wires.wait(7, every(moved(me, "c", 1)["c"]), me)

    def s5():
        me = here()
        for j in range(3):
            wires.sent(j, source, me)
        for i, c in ((3, cols), (4, cols), (5, left), (6, right)):
            wires.sent(i, row(me, c), me)
        wires.sent(7, every(me["c"]), me)

    return [s0, s1, s2, s3, s4, s5]


SUM_PEERS = (("c", 1), *((axis, step) for axis in "xyz" for step in (1, 2, 3)))
SUM_SEMS = 20
SUM_ORDERS = ("xyz", "yzx", "zxy")


def sum_scratch(rows, columns):
    w = columns // 4
    vm = lambda *shape: pltpu.VMEM((*shape, rows, w), BF16)
    wide = lambda *shape: pltpu.VMEM((*shape, rows, w), F32)
    return [
        *[pltpu.VMEM((4, 4, rows, columns), BF16)] * 2,
        vm(2, 8), vm(2, 8), vm(2, 16), vm(2, 16), wide(16),
        vm(2, 2), vm(2, 2), vm(2, 4), vm(2, 4), wide(4),
        vm(3), vm(3), vm(4),
        pltpu.SemaphoreType.DMA((12,)), pltpu.SemaphoreType.DMA((SUM_SEMS,)), pltpu.SemaphoreType.DMA((SUM_SEMS,)),
    ]


SUM_REFS = 18


def sum_stages(order, term, there, out, refs):
    own, mates, o1, i1, o2, i2, k1, o3, i3, o4, i4, k2, o5, i5, ob, local, send, recv = refs
    wires = Wires(send, recv)
    A, B, D = order
    w = out.shape[-1] // 4

    def lane(q):
        return pl.ds(pl.multiple_of(q * w, 128), w)

    def chip(p):
        at = p["y"], p["z"], slice(None), lane(p["x"])
        return own[at].astype(F32) + mates[at].astype(F32)

    QUARTERS = (2, 1, 3, 0)

    def quarter(ref, me, k, core=None):
        n = lax.rem(me[A] + QUARTERS[k], 4)
        y, z, x = (n if A == axis else slice(None) for axis in "yzx")
        cols = lane(n) if A == "x" else slice(None)
        return ref.at[y, z, :, cols] if core is None else ref.at[y, z, core, :, cols]

    def fetch(me, k):
        return pltpu.make_async_copy(quarter(term, me, k, me["c"]), quarter(own, me, k), local.at[k])

    def fetch_mates(me, k):
        return pltpu.make_async_copy(quarter(there, me, k), quarter(mates, me, k), local.at[8 + k])

    def r0():
        me = here()
        mate = moved(me, "c", 1)
        for k in range(4):
            if there is None:
                wires.go(k, quarter(term, me, k, mate["c"]), quarter(mates, me, k), mate)
            else:
                fetch_mates(me, k).start()
            fetch(me, k).start()

    def have(me, k):
        fetch(me, k).wait()
        if there is None:
            wires.wait(k, quarter(mates, me, k), me)
        else:
            fetch_mates(me, k).wait()

    def r1():
        me = here()
        have(me, 0)
        far = lax.rem(me[A] + 2, 4)
        for turn, step in ((0, 1), (1, 3)):

            @pl.loop(0, 8)
            def _(i):
                b, d = lax.div(i, 4), lax.rem(i, 4)
                o1[turn, i] = chip({A: far, B: 2 * turn + b, D: d}).astype(BF16)

            wires.go(4 + turn, o1.at[turn], i1.at[turn], moved(me, A, step))
        for turn, step in ((0, 1), (1, 3)):
            to = moved(me, A, step)
            have(me, 1 + turn)

            @pl.loop(0, 8)
            def _(i):
                b, d = lax.div(i, 4), lax.rem(i, 4)
                o2[turn, 8 * (1 - turn) + i] = chip({A: to[A], B: 2 * (1 - turn) + b, D: d}).astype(BF16)

            rest = pl.ds(8 * (1 - turn), 8)
            wires.go(18 + turn, o2.at[turn, rest], i2.at[turn, rest], to)

    def r2():
        me = here()
        for turn, step in ((0, 1), (1, 3)):
            wires.wait(4 + turn, i1.at[turn], me)
            to = moved(me, A, step)

            @pl.loop(0, 8)
            def _(i):
                b, d = lax.div(i, 4), lax.rem(i, 4)
                o2[turn, 8 * turn + i] = (chip({A: to[A], B: 2 * turn + b, D: d}) + i1[turn, i].astype(F32)).astype(BF16)

            added = pl.ds(8 * turn, 8)
            wires.go(6 + turn, o2.at[turn, added], i2.at[turn, added], to)

    def r3():
        me = here()
        have(me, 3)
        for turn in (0, 1):
            wires.wait(18 + turn, i2.at[turn, pl.ds(8 * (1 - turn), 8)], me)
            wires.wait(6 + turn, i2.at[turn, pl.ds(8 * turn, 8)], me)

        @pl.loop(0, 16)
        def _(i):
            k1[i] = chip({A: me[A], B: lax.div(i, 4), D: lax.rem(i, 4)}) + i2[0, i].astype(F32) + i2[1, i].astype(F32)

        far = lax.rem(me[B] + 2, 4)
        for turn, step in ((0, 1), (1, 3)):
            for d in range(2):
                o3[turn, d] = k1[far * 4 + 2 * turn + d].astype(BF16)
            wires.go(8 + turn, o3.at[turn], i3.at[turn], moved(me, B, step))

    def r4():
        me = here()
        for turn, step in ((0, 1), (1, 3)):
            wires.wait(8 + turn, i3.at[turn], me)
            to = moved(me, B, step)
            for d in range(2):
                o4[turn, 2 * turn + d] = (k1[to[B] * 4 + 2 * turn + d] + i3[turn, d].astype(F32)).astype(BF16)
                o4[turn, 2 * (1 - turn) + d] = k1[to[B] * 4 + 2 * (1 - turn) + d].astype(BF16)
            wires.go(10 + turn, o4.at[turn], i4.at[turn], to)

    def r5():
        me = here()
        for turn in (0, 1):
            wires.wait(10 + turn, i4.at[turn], me)
        for d in range(4):
            k2[d] = k1[me[B] * 4 + d] + i4[0, d].astype(F32) + i4[1, d].astype(F32)
        for j in (1, 2, 3):
            to = moved(me, D, j)
            o5[j - 1] = k2[to[D]].astype(BF16)
            wires.go(11 + j, o5.at[j - 1], i5.at[j - 1], to)

    def r6():
        me = here()
        total = k2[me[D]]
        for j in (1, 2, 3):
            wires.wait(11 + j, i5.at[j - 1], me)
            total = total + i5[j - 1].astype(F32)
        ob[me["x"]] = total.astype(BF16)
        for j in (1, 2, 3):
            wires.go(14 + j, ob.at[me["x"]], ob.at[me["x"]], moved(me, "x", j))

    def put(q):
        return pltpu.make_async_copy(ob.at[q], out.at[:, pl.ds(q * w, w)], local.at[4 + q])

    def r7():
        me = here()
        for j in (1, 2, 3):
            wires.wait(14 + j, ob.at[moved(me, "x", 4 - j)["x"]], me)
        for q in range(4):
            put(q).start()
        for k in range(4):
            if there is None:
                wires.sent(k, quarter(mates, me, k), me)
        for turn in (0, 1):
            wires.sent(4 + turn, o1.at[turn], me)
            wires.sent(6 + turn, o2.at[turn, pl.ds(8 * turn, 8)], me)
            wires.sent(18 + turn, o2.at[turn, pl.ds(8 * (1 - turn), 8)], me)
            wires.sent(8 + turn, o3.at[turn], me)
            wires.sent(10 + turn, o4.at[turn], me)
        for j in (1, 2, 3):
            wires.sent(11 + j, o5.at[j - 1], me)
            wires.sent(14 + j, ob.at[me["x"]], me)
        for q in range(4):
            put(q).wait()

    return [r0, r1, r2, r3, r4, r5, r6, r7]


def cut(term):
    return term.reshape(4, 4, 2, term.shape[0] // 32, term.shape[1])


class Mates(Exchange):
    peers = (("c", 1),)

    def __init__(self, terms):
        self.operands = [cut(t) for t in terms]
        self.in_specs = [ANY] * len(terms)
        self.out_shape = [jax.ShapeDtypeStruct((4, 4, *t.shape[3:]), BF16) for t in self.operands]
        self.out_specs = [ANY] * len(terms)
        self.scratch = [pltpu.SemaphoreType.DMA((len(terms),))] * 2

    def plan(self, ins, outs, scratch):
        wires = Wires(*scratch)

        def begin():
            mate = moved(here(), "c", 1)
            for n, (term, out) in enumerate(zip(ins, outs, strict=True)):
                wires.go(n, term.at[:, :, mate["c"]], out, mate)

        def end():
            me = here()
            for n, out in enumerate(outs):
                wires.wait(n, out, me)
                wires.sent(n, out, me)

        return [[begin, end]]


MATES_MARKS = {0: [(0, 0)], "end": [(0, 1)]}


class Sum(Exchange):
    peers = SUM_PEERS

    def __init__(self, terms, mates=()):
        self.n = len(terms)
        terms = [cut(t) for t in terms]
        self.operands = [*terms, *mates]
        self.in_specs = [ANY] * len(self.operands)
        self.out_shape = [jax.ShapeDtypeStruct(t.shape[3:], BF16) for t in terms]
        self.out_specs = [ANY] * self.n
        self.scratch = [s for t in terms for s in sum_scratch(*t.shape[3:])]

    def plan(self, ins, outs, scratch):
        theres = list(ins[self.n :]) or [None] * self.n
        return [sum_stages(SUM_ORDERS[i], ins[i], theres[i], outs[i], scratch[SUM_REFS * i : SUM_REFS * (i + 1)]) for i in range(self.n)]


def all_of(*numbers):
    return [(which, number) for number in numbers for which in range(3)]


SUM_LONG_MARKS = {0: all_of(0), 1: all_of(1), 3: all_of(2), 5: all_of(3), 6: all_of(4), 7: all_of(5), 8: all_of(6), "end": all_of(7)}
SUM_SHORT_MARKS = {0: all_of(0), 1: all_of(1), 4: all_of(2), 7: all_of(3), "end": all_of(4, 5, 6, 7)}


def dot(a, b, dims=((1,), (0,))):
    return lax.dot_general(a, b, (dims, ((), ())), preferred_element_type=F32)


def scale_of(wide):
    return lax.rsqrt(jnp.mean(wide * wide, -1, keepdims=True) + 1e-6)


def norm_into(h, a, at, chunk=512):
    @pl.loop(0, h.shape[0], step=chunk)
    def _(m):
        rows = pl.ds(m, chunk)
        wide = h[rows, :].astype(F32)
        value = (wide * scale_of(wide)).astype(BF16)
        if a is not None:
            a[rows, :] = value
        if at is not None:
            at[:, rows] = value.T


def whole(shape):
    return pl.BlockSpec(shape, lambda i: (0,) * len(shape), pipeline_mode=pl.Buffered(1))


TILE, CHUNK = 256, 512


def call(kernel, grid, operands, in_specs, out_shape, out_specs, scratch, name, exchange=None, marks=None, collective_id=None):
    counts = [len(operands), len(out_shape), len(scratch)]
    extra = [exchange.operands, exchange.out_shape, exchange.scratch] if exchange else [[], [], []]
    n_extra = [len(e) for e in extra]

    def body(*refs):
        refs, mine, theirs = list(refs), [], []
        for n, k in zip(counts, n_extra, strict=True):
            mine += refs[:n]
            theirs.append(refs[n : n + k])
            refs = refs[n + k :]
        i = pl.program_id(0)
        if exchange:
            plan = exchange.plan(*theirs)
            exchange.grid_step(plan, marks, i)
        kernel(*mine)
        if exchange:

            @pl.when(i == grid - 1)
            def _():
                exchange.finish(plan, marks)

    params = dict(collective_id=collective_id, has_side_effects=True) if exchange else {}
    out = pl.pallas_call(
        body,
        grid=(grid,),
        out_shape=list(out_shape) + (exchange.out_shape if exchange else []),
        in_specs=list(in_specs) + (exchange.in_specs if exchange else []),
        out_specs=list(out_specs) + (exchange.out_specs if exchange else []),
        scratch_shapes=list(scratch) + (exchange.scratch if exchange else []),
        compiler_params=pltpu.CompilerParams(vmem_limit_bytes=LIMIT, **params),
        name=name,
    )(*operands, *(exchange.operands if exchange else []))
    return out[: counts[1]], out[counts[1] :]


PIECES = ((0, 256, 0), (256, 256, 1), (512, 512, 2), (1024, 512, 4), (1536, 512, 6), (2048, 512, 8))
DOWN_AT = (-4, -2, -1, 0, 1, 5, 7, 9)
NEXT_DOWN_AT = (1, 2, 3, 4, 6, 10, 12, 99)
NEXT_AT = (5, 6, 7, 10, 11, 99)
EARLY = 1024


def forward(h, weights, collective_id):
    tokens, d = h.shape
    ff = weights[0].shape[2]
    tiles, outs = ff // TILE, d // TILE
    steps = tiles + outs
    pieces = len(PIECES)
    now = [jax.ShapeDtypeStruct(w.shape[1:], BF16) for w in weights]
    later = [jax.ShapeDtypeStruct((w.shape[1], EARLY), BF16) for w in weights[:2]] + now[2:]
    next_layer = Gather(later)

    def kernel(h_ref, wg_ref, wu_ref, wd_ref, y_ref, g_ref, u_ref, at_ref, fg, fu, fd, hg, hu, hd, a, act, vg, vu, vd, local, csend, crecv, dsend, drecv, *scratch):
        i = pl.program_id(0)
        ng, nu, nd = wg_ref.at[0], wu_ref.at[0], wd_ref.at[0]
        lg, lu, ld = wg_ref.at[1, :, pl.ds(0, EARLY)], wu_ref.at[1, :, pl.ds(0, EARLY)], wd_ref.at[1]
        todo = {}

        def plan(at, stages):
            for k, stage in zip(at, stages):
                todo.setdefault(min(k, steps), []).append(stage)

        def keep(n, src, dst):
            return pltpu.make_async_copy(src, dst, local.at[2 * pieces + 1 + n])

        matrices = ((("z", "y"), ng, vg), (("y", "z"), nu, vu))
        for k in reversed(range(pieces)):
            start, size, need = PIECES[k]
            for m, (order, w, full) in enumerate(matrices):
                n = m * pieces + k
                if k == 0:
                    plan((-4, -1, 0, 99), gather_stages_direct(w, full, local.at[n], dsend.at[m], drecv.at[m], start, size))
                else:
                    plan((*range(need - 4, need + 1), 99), gather_stages_chunk(*order, w, full, local.at[n], csend.at[n], crecv.at[n], start, size))
        plan(DOWN_AT, gather_stages_x("z", "y", nd, vd, local.at[2 * pieces], dsend.at[2], drecv.at[2]))
        plan((tiles, tiles, tiles, 99, 99, 99), [keep(0, vg, fg).start, keep(1, vu, fu).start, keep(2, vd, fd).start, keep(0, vg, fg).wait, keep(1, vu, fu).wait, keep(2, vd, fd).wait])
        after = next_layer.plan((lg, lu, ld), (hg, hu, hd), scratch)
        for which, at in enumerate((NEXT_AT, NEXT_AT, NEXT_DOWN_AT)):
            plan(at, after[which])

        @pl.when(i == 0)
        def _():
            greet(PLANE_PEERS)
            for t in sorted(todo):
                if t < 0:
                    for f in todo[t]:
                        f()
                if t == -3:
                    norm_into(h_ref, a, at_ref)

        for at in range(steps):
            if at in todo:

                @pl.when(i == at)
                def _():
                    for f in todo[at]:
                        f()

        @pl.when(i < tiles)
        def _():
            cols = pl.ds(pl.multiple_of(i * TILE, TILE), TILE)
            wg = vg[:, :, :, :, cols].reshape(d, TILE)
            wu = vu[:, :, :, :, cols].reshape(d, TILE)

            @pl.loop(0, tokens, step=CHUNK)
            def _(m):
                rows = pl.ds(m, CHUNK)
                g = dot(a[rows, :], wg)
                u = dot(a[rows, :], wu)
                g_ref[rows, :] = g
                u_ref[rows, :] = u
                act[i, rows, :] = (g * jax.nn.sigmoid(g) * u).astype(BF16)

        @pl.when(i >= tiles)
        def _():
            cols = pl.ds(pl.multiple_of((i - tiles) * TILE, TILE), TILE)

            @pl.loop(0, tokens, step=CHUNK)
            def _(m):
                rows = pl.ds(m, CHUNK)
                total = sum(dot(act[k, rows, :], vd[:, :, :, :, cols].reshape(ff, TILE)[k * TILE : (k + 1) * TILE, :]) for k in range(tiles))
                y_ref[rows, :] = h_ref[rows, cols] + total.astype(BF16)

        @pl.when(i == steps - 1)
        def _():
            for f in todo[steps]:
                f()

    tile = pl.BlockSpec((tokens, TILE), lambda i: (0, jnp.minimum(i, tiles - 1)))
    full_types = [jax.ShapeDtypeStruct(blocks_of(w), BF16) for w in (*now, *later)]
    dma = pltpu.SemaphoreType.DMA
    out = pl.pallas_call(
        kernel,
        grid=(steps,),
        out_shape=[
            jax.ShapeDtypeStruct(h.shape, BF16),
            jax.ShapeDtypeStruct((tokens, ff), F32),
            jax.ShapeDtypeStruct((tokens, ff), F32),
            jax.ShapeDtypeStruct((d, tokens), BF16),
            *full_types,
        ],
        in_specs=[whole(h.shape)] + [whole(w.shape) for w in weights],
        out_specs=[pl.BlockSpec((tokens, TILE), lambda i: (0, jnp.maximum(i - tiles, 0))), tile, tile, whole((d, tokens))] + [ANY] * 6,
        scratch_shapes=[
            pltpu.VMEM(h.shape, BF16),
            pltpu.VMEM((tiles, tokens, TILE), BF16),
            *(pltpu.VMEM(t.shape, BF16) for t in full_types[:3]),
            dma((2 * pieces + 4,)),
            dma((2 * pieces, 8)),
            dma((2 * pieces, 8)),
            dma((3, 16)),
            dma((3, 16)),
            *next_layer.scratch,
        ],
        compiler_params=pltpu.CompilerParams(vmem_limit_bytes=LIMIT, collective_id=collective_id, has_side_effects=True),
        name="forward",
    )(h, *weights)
    return out[:4], [f.reshape(-1, f.shape[-1]) for f in out[4:]]


def hidden_grads(g, u, by_act):
    sig = jax.nn.sigmoid(g)
    silu = g * sig
    by_act = by_act.astype(BF16).astype(F32)
    return (silu * u).astype(BF16), (by_act * u * (sig * (1 + g * (1 - sig)))).astype(BF16), (by_act * silu).astype(BF16)


def backward_fresh(h, by_y, early, weights, wd, collective_id):
    tokens, d = h.shape
    ff = wd.shape[0]
    steps, first = ff // TILE, EARLY // TILE
    late = ff - EARLY

    def kernel(h_ref, ga, ua, wg_ref, wu_ref, by_ref, wd_ref, dg_ref, du_ref, dwg_ref, dwu_ref, dwd_ref, hg, hu, a, at, act, tg, tu, vg, vu, local, send, recv):
        i = pl.program_id(0)
        lists = [
            gather_stages_chunk(*order, w.at[1], full, local.at[n], send.at[n], recv.at[n], EARLY, late, 0)
            for n, (order, w, full) in enumerate(((("z", "y"), wg_ref, vg), (("y", "z"), wu_ref, vu)))
        ]
        keep = [pltpu.make_async_copy(v, o, local.at[2 + n]) for n, (v, o) in enumerate(((vg, hg), (vu, hu)))]

        for at_step in range(first + 1):

            @pl.when(i == at_step)
            def _():
                if at_step == 0:
                    greet(Gather.peers)
                for stages in lists:
                    stages[at_step]()
                if at_step == 0:
                    norm_into(h_ref, a, at)
                if at_step == first:
                    for k in keep:
                        k.start()

        @pl.when(i < first)
        def _():
            cols = pl.ds(pl.multiple_of(i * TILE, TILE), TILE)
            tg[...] = ga[:, cols]
            tu[...] = ua[:, cols]

        @pl.when(i >= first)
        def _():
            cols = pl.ds(pl.multiple_of((i - first) * TILE, TILE), TILE)
            tg[...] = vg[:, :, :, :, cols].reshape(d, TILE)
            tu[...] = vu[:, :, :, :, cols].reshape(d, TILE)

        @pl.loop(0, tokens, step=CHUNK)
        def _(m):
            rows = pl.ds(m, CHUNK)
            g, u = dot(a[rows, :], tg[...]), dot(a[rows, :], tu[...])
            by_act = dot(by_ref[rows, :], wd_ref[...], ((1,), (1,)))
            act[rows, :], dg_ref[rows, :], du_ref[rows, :] = hidden_grads(g, u, by_act)

        dwd_ref[...] = dot(act[...], by_ref[...], ((0,), (0,))).astype(BF16)
        dwg_ref[...] = dot(at[...], dg_ref[...]).astype(BF16)
        dwu_ref[...] = dot(at[...], du_ref[...]).astype(BF16)

        @pl.when(i == steps - 1)
        def _():
            for stages in lists:
                stages[5]()
            for k in keep:
                k.wait()

    across = pl.BlockSpec((d, TILE), lambda i: (0, i))
    down = pl.BlockSpec((TILE, d), lambda i: (i, 0))
    tile = pl.BlockSpec((tokens, TILE), lambda i: (0, i))
    part = (4, 4, 2, d // 32, late)
    dma = pltpu.SemaphoreType.DMA
    out = pl.pallas_call(
        kernel,
        grid=(steps,),
        out_shape=[jax.ShapeDtypeStruct((tokens, ff), BF16)] * 2
        + [jax.ShapeDtypeStruct((d, ff), BF16)] * 2
        + [jax.ShapeDtypeStruct((ff, d), BF16)]
        + [jax.ShapeDtypeStruct(part, BF16)] * 2,
        in_specs=[whole((tokens, d)), *[whole((d, EARLY))] * 2, *[whole(w.shape) for w in weights[:2]], whole((tokens, d)), down],
        out_specs=[tile, tile, across, across, down, ANY, ANY],
        scratch_shapes=[
            pltpu.VMEM((tokens, d), BF16),
            pltpu.VMEM((d, tokens), BF16),
            pltpu.VMEM((tokens, TILE), BF16),
            *[pltpu.VMEM((d, TILE), BF16)] * 2,
            *[pltpu.VMEM(part, BF16)] * 2,
            dma((4,)),
            dma((2, 8)),
            dma((2, 8)),
        ],
        compiler_params=pltpu.CompilerParams(vmem_limit_bytes=LIMIT, collective_id=collective_id, has_side_effects=True),
        name="backward_fresh",
    )(h, *early, *weights[:2], by_y, wd)
    return out[:2], out[2:5], [f.reshape(d, late) for f in out[5:]]


def backward_hidden(by_y, wd, saved, **beside):
    tokens, d = by_y.shape
    ff = wd.shape[0]
    steps = ff // TILE

    def kernel(at, g_ref, u_ref, by_ref, wd_ref, dg_ref, du_ref, dwg_ref, dwu_ref, dwd_ref, act):
        @pl.loop(0, tokens, step=CHUNK)
        def _(m):
            rows = pl.ds(m, CHUNK)
            by_act = dot(by_ref[rows, :], wd_ref[...], ((1,), (1,)))
            act[rows, :], dg_ref[rows, :], du_ref[rows, :] = hidden_grads(g_ref[rows, :], u_ref[rows, :], by_act)

        dwd_ref[...] = dot(act[...], by_ref[...], ((0,), (0,))).astype(BF16)
        dwg_ref[...] = dot(at[...], dg_ref[...]).astype(BF16)
        dwu_ref[...] = dot(at[...], du_ref[...]).astype(BF16)

    across = pl.BlockSpec((d, TILE), lambda i: (0, i))
    down = pl.BlockSpec((TILE, d), lambda i: (i, 0))
    tile = pl.BlockSpec((tokens, TILE), lambda i: (0, i))
    return call(
        kernel,
        steps,
        (*saved, by_y, wd),
        [whole((d, tokens)), tile, tile, whole((tokens, d)), down],
        [jax.ShapeDtypeStruct((tokens, ff), BF16)] * 2 + [jax.ShapeDtypeStruct((d, ff), BF16)] * 2 + [jax.ShapeDtypeStruct((ff, d), BF16)],
        [tile, tile, across, across, down],
        [pltpu.VMEM((tokens, TILE), BF16)],
        "backward_hidden",
        **beside,
    )


def backward_input(dg, du, wgs, wus, h, by_y, **beside):
    tokens, d = h.shape
    ff = dg.shape[1]
    chunk = 256

    n = len(wgs)

    def kernel(dg_ref, du_ref, *refs):
        parts, (h_ref, by_ref, out_ref) = refs[: 2 * n], refs[2 * n :]
        by_a, start = 0, 0
        for wg_ref, wu_ref in zip(parts[:n], parts[n:], strict=True):
            cols = pl.ds(start, wg_ref.shape[1])
            start += wg_ref.shape[1]
            by_a = by_a + dot(dg_ref[:, cols], wg_ref[...], ((1,), (1,))) + dot(du_ref[:, cols], wu_ref[...], ((1,), (1,)))
        by_a = by_a.astype(BF16).astype(F32)
        wide = h_ref[...].astype(F32)
        scale = scale_of(wide)
        back = jnp.sum(by_a * wide, -1, keepdims=True) * (scale * scale * scale) * (1 / d)
        out_ref[...] = by_ref[...] + (by_a * scale - wide * back).astype(BF16)

    rows = lambda n: pl.BlockSpec((chunk, n), lambda i: (i, 0))
    return call(
        kernel,
        tokens // chunk,
        (dg, du, *wgs, *wus, h, by_y),
        [rows(ff), rows(ff), *(whole(w.shape) for w in (*wgs, *wus)), rows(d), rows(d)],
        [jax.ShapeDtypeStruct(h.shape, BF16)],
        [rows(d)],
        [],
        "backward_input",
        **beside,
    )


def stacked(layers):
    n = len(layers[0])

    def kernel(*refs):
        for k in range(n):
            for layer in range(len(layers)):
                refs[len(layers) * n + k][layer] = refs[layer * n + k][...]

    return pl.pallas_call(
        kernel,
        out_shape=[jax.ShapeDtypeStruct((len(layers), *t.shape), BF16) for t in layers[0]],
        name="stacked",
    )(*(t for layer in layers for t in layer))


def solution(mesh):
    def step(x, dy, *weights):
        x, dy = x[0], dy[0]
        (h1, g0, u0, at0), (wg0, wu0, wd0, wg1, wu1, wd1) = forward(x, weights, 1)
        (dg1, du1), terms1, (wg1_rest, wu1_rest) = backward_fresh(h1, dy, (wg1, wu1), weights, wd1, 2)
        (by_h1,), mates1 = backward_input(dg1, du1, (wg1, wg1_rest), (wu1, wu1_rest), h1, dy, exchange=Mates(terms1), marks=MATES_MARKS, collective_id=3)
        (dg0, du0, *terms0), sums1 = backward_hidden(by_h1, wd0, (at0, g0, u0), exchange=Sum(terms1, mates1), marks=SUM_LONG_MARKS, collective_id=4)
        (by_x,), sums0 = backward_input(dg0, du0, (wg0,), (wu0,), x, by_h1, exchange=Sum(terms0), marks=SUM_SHORT_MARKS, collective_id=5)
        return (by_x[None], *stacked([sums0, sums1]))

    states, shard = P(("rep", "r", "s"), None, None), P(None, "s", None)
    return jax.shard_map(
        step,
        mesh=mesh,
        in_specs=(states, states) + (shard,) * 3,
        out_specs=(states,) + (P("rep", "s", None),) * 3,
        check_vma=False,
    )
```

```python
import functools

import jax
import jax.numpy as jnp
from jax import lax
from jax.experimental import pallas as pl
from jax.experimental.pallas import tpu as pltpu
from jax.sharding import PartitionSpec as P

F32, BF16 = jnp.float32, jnp.bfloat16
MESH = pl.DeviceIdType.MESH
ANY = pl.BlockSpec(memory_space=pl.ANY)
LIMIT = 66_000_000
SIZE = {"x": 4, "y": 4, "z": 4, "c": 2}


def here():
    s = lax.axis_index("s")
    return {"x": lax.axis_index("r"), "y": lax.div(s, 8), "z": lax.rem(lax.div(s, 2), 4), "c": lax.rem(s, 2)}


def moved(p, axis, step):
    return {**p, axis: lax.rem(p[axis] + step, SIZE[axis])}


def device(p):
    return {"r": p["x"], "s": (p["y"] * 4 + p["z"]) * 2 + p["c"]}


def greet(peers):
    me = here()
    barrier = pltpu.get_barrier_semaphore()
    for peer in peers:
        to = me
        for axis, step in peer if isinstance(peer[0], tuple) else (peer,):
            to = moved(to, axis, step)
        pl.semaphore_signal(barrier, inc=1, device_id=device(to), device_id_type=MESH)
    pl.semaphore_wait(barrier, len(peers))


class Wires:
    def __init__(self, send, recv):
        self.send, self.recv, self.pending = send, recv, []

    def go(self, i, src, dst, to):
        copy = lambda: pltpu.make_async_remote_copy(src, dst, self.send.at[i], self.recv.at[i], device_id=device(to), device_id_type=MESH)
        copy().start()

    def sent(self, i, src, to):
        pltpu.make_async_remote_copy(src, src, self.send.at[i], self.recv.at[i], device_id=device(to), device_id_type=MESH).wait_send()

    def wait(self, i, dst, to):
        pltpu.make_async_remote_copy(dst, dst, self.send.at[i], self.recv.at[i], device_id=device(to), device_id_type=MESH).wait_recv()


def gather_stages(first, second, w, full, local, send, recv):
    wires = Wires(send, recv)
    half = w.shape[-1] // 2
    left, right = pl.ds(0, half), pl.ds(half, half)

    def block(p, **free):
        p = {**p, **free}
        return full.at[p["y"], p["z"], p["c"]]

    def row(p, cols=None):
        p = {**p, first: slice(None)}
        return full.at[p["y"], p["z"], p["c"]] if cols is None else full.at[p["y"], p["z"], p["c"], :, cols]

    def part(p, cols):
        return full.at[p["y"], p["z"], p["c"], :, cols]

    def s0():
        me = here()
        pltpu.make_async_copy(w, block(me), local).start()
        wires.go(0, w, block(me), moved(me, first, 1))
        wires.go(1, w, block(me), moved(me, first, 3))

    def s1():
        me = here()
        before, after = moved(me, first, 3), moved(me, first, 1)
        wires.wait(0, block(before), before)
        wires.go(2, part(before, left), part(before, left), after)
        wires.wait(1, block(after), after)
        wires.go(3, part(after, right), part(after, right), before)
        pltpu.make_async_copy(w, block(me), local).wait()

    def s2():
        me = here()
        far = moved(me, first, 2)
        wires.wait(2, part(far, left), me)
        wires.wait(3, part(far, right), me)
        for i, (axis, step) in ((4, (second, 1)), (5, (second, 3)), (8, ("c", 1))):
            wires.go(i, row(me), row(me), moved(me, axis, step))

    def s3():
        me = here()
        before, after, mate = moved(me, second, 3), moved(me, second, 1), moved(me, "c", 1)
        wires.wait(4, row(before), before)
        wires.go(6, row(before, left), row(before, left), after)
        wires.wait(5, row(after), after)
        wires.go(7, row(after, right), row(after, right), before)
        wires.go(9, row(before), row(before), mate)
        wires.go(10, row(after), row(after), mate)

    def s4():
        me = here()
        far, mate = moved(me, second, 2), moved(me, "c", 1)
        wires.wait(6, row(far, left), me)
        wires.wait(7, row(far, right), me)
        wires.go(11, row(far), row(far), mate)

    def s5():
        me = here()
        mate = moved(me, "c", 1)
        for i, step in ((8, 0), (9, 3), (10, 1), (11, 2)):
            wires.wait(i, row(moved(mate, second, step)), me)
        for i in (0, 1):
            wires.sent(i, w, me)
        for i, cols in ((2, left), (3, right)):
            wires.sent(i, part(me, cols), me)
        for i in (4, 5, 8, 9, 10, 11):
            wires.sent(i, row(me), me)
        for i, cols in ((6, left), (7, right)):
            wires.sent(i, row(me, cols), me)

    return [s0, s1, s2, s3, s4, s5]


def gather_stages_x(first, second, w, full, local, send, recv):
    wires = Wires(send, recv)
    quarter = w.shape[-1] // 4
    half = quarter // 2

    def cols(q, at=0, size=quarter):
        return pl.ds(pl.multiple_of(q * quarter + at, half), size)

    def part(p, c, **free):
        p = {**p, **free}
        return full.at[p["y"], p["z"], p["c"], :, c]

    def row(p, c):
        return part(p, c, **{first: slice(None)})

    def plane(p, q, ys=slice(None)):
        return full.at[ys, :, p["c"], :, cols(q)]

    def halves(me):
        return cols(me["x"], 0, half), cols(me["x"], half, half)

    def s0():
        me = here()
        q = cols(me["x"])
        pltpu.make_async_copy(w.at[:, q], part(me, q), local).start()
        wires.go(0, w.at[:, q], part(me, q), moved(me, first, 1))
        wires.go(1, w.at[:, q], part(me, q), moved(me, first, 3))

    def s1():
        me = here()
        q, (left, right) = cols(me["x"]), halves(me)
        before, after = moved(me, first, 3), moved(me, first, 1)
        wires.wait(0, part(before, q), before)
        wires.go(2, part(before, left), part(before, left), after)
        wires.wait(1, part(after, q), after)
        wires.go(3, part(after, right), part(after, right), before)
        pltpu.make_async_copy(w.at[:, q], part(me, q), local).wait()

    def s2():
        me = here()
        q, (left, right) = cols(me["x"]), halves(me)
        far = moved(me, first, 2)
        wires.wait(2, part(far, left), me)
        wires.wait(3, part(far, right), me)
        wires.go(4, row(me, q), row(me, q), moved(me, second, 1))
        wires.go(5, row(me, q), row(me, q), moved(me, second, 3))

    def s3():
        me = here()
        q, (left, right) = cols(me["x"]), halves(me)
        before, after = moved(me, second, 3), moved(me, second, 1)
        wires.wait(4, row(before, q), before)
        wires.go(6, row(before, left), row(before, left), after)
        wires.wait(5, row(after, q), after)
        wires.go(7, row(after, right), row(after, right), before)

    def s4():
        me = here()
        left, right = halves(me)
        far = moved(me, second, 2)
        wires.wait(6, row(far, left), me)
        wires.wait(7, row(far, right), me)
        q = me["x"]
        for i, (axis, step) in ((8, ("x", 1)), (9, ("x", 3)), (12, ("c", 1))):
            wires.go(i, plane(me, q), plane(me, q), moved(me, axis, step))

    low, high = slice(0, 2), slice(2, 4)

    def s5():
        me = here()
        before, after, mate = moved(me, "x", 3), moved(me, "x", 1), moved(me, "c", 1)
        wires.wait(8, plane(me, before["x"]), me)
        wires.go(10, plane(me, before["x"], low), plane(me, before["x"], low), after)
        wires.wait(9, plane(me, after["x"]), me)
        wires.go(11, plane(me, after["x"], high), plane(me, after["x"], high), before)
        wires.go(13, plane(me, before["x"]), plane(me, before["x"]), mate)
        wires.go(14, plane(me, after["x"]), plane(me, after["x"]), mate)

    def s6():
        me = here()
        far, mate = moved(me, "x", 2)["x"], moved(me, "c", 1)
        wires.wait(10, plane(me, far, low), me)
        wires.wait(11, plane(me, far, high), me)
        wires.go(15, plane(me, far), plane(me, far), mate)

    def s7():
        me = here()
        mate = moved(me, "c", 1)
        q, (left, right) = cols(me["x"]), halves(me)
        for i, step in ((12, 0), (13, 3), (14, 1), (15, 2)):
            wires.wait(i, plane(mate, moved(me, "x", step)["x"]), me)
        for i in (0, 1):
            wires.sent(i, w.at[:, q], me)
        for i, c in ((2, left), (3, right)):
            wires.sent(i, part(me, c), me)
        for i, c in ((4, q), (5, q), (6, left), (7, right)):
            wires.sent(i, row(me, c), me)
        for i in (8, 9, 12, 13, 14, 15):
            wires.sent(i, plane(me, me["x"]), me)
        for i, ys in ((10, low), (11, high)):
            wires.sent(i, plane(me, me["x"], ys), me)

    return [s0, s1, s2, s3, s4, s5, s6, s7]


def gather_stages_direct(w, full, local, send, recv, start, size):
    wires = Wires(send, recv)
    cols = pl.ds(start, size)
    others = [(j, k) for j in (1, 3, 0, 2) for k in (1, 3, 0, 2) if (j, k) != (0, 0)]

    def part(p):
        return full.at[p["y"], p["z"], p["c"], :, cols]

    def every(c):
        return full.at[:, :, c, :, cols]

    def s0():
        me = here()
        for n, (j, k) in enumerate(others):
            wires.go(n, w.at[:, cols], part(me), moved(moved(me, "y", j), "z", k))
        pltpu.make_async_copy(w.at[:, cols], part(me), local).start()

    def s1():
        me = here()
        pltpu.make_async_copy(w.at[:, cols], part(me), local).wait()
        for n, (j, k) in enumerate(others):
            wires.wait(n, part(moved(moved(me, "y", 4 - j), "z", 4 - k)), me)
        wires.go(15, every(me["c"]), every(me["c"]), moved(me, "c", 1))

    def s2():
        wires.wait(15, every(moved(here(), "c", 1)["c"]), here())

    def s3():
        me = here()
        for n in range(15):
            wires.sent(n, w.at[:, cols], me)
        wires.sent(15, every(me["c"]), me)

    return [s0, s1, s2, s3]


def blocks_of(w):
    return (4, 4, 2, w.shape[0], w.shape[1])


PLANE_PEERS = (("c", 1), ("x", 1), ("x", 3), *((("y", j), ("z", k)) for j in range(4) for k in range(4) if j or k))


class Exchange:
    def before(self):
        greet(self.peers)

    def grid_step(self, plan, marks, i):
        for at, steps in marks.items():
            if at != "end":

                @pl.when(i == at)
                def _():
                    if at == 0:
                        self.before()
                    for which, number in steps:
                        plan[which][number]()

    def finish(self, plan, marks):
        for which, number in marks["end"]:
            plan[which][number]()


class Gather(Exchange):
    peers = (("c", 1), *((axis, step) for axis in "yz" for step in (1, 2, 3)), ("x", 1), ("x", 3))

    def __init__(self, ws):
        n = len(ws)
        self.operands = list(ws)
        self.in_specs = [pl.BlockSpec(memory_space=pltpu.VMEM)] * n
        self.out_shape = [jax.ShapeDtypeStruct(blocks_of(w), BF16) for w in ws]
        self.out_specs = [ANY] * n
        sems = [12, 12, 16]
        self.scratch = [pltpu.SemaphoreType.DMA((n,))] + [pltpu.SemaphoreType.DMA((k,)) for k in sems for _ in range(2)]

    def plan(self, ins, outs, scratch):
        local, *sems = scratch
        makers = (functools.partial(gather_stages, "z", "y"), functools.partial(gather_stages, "y", "z"), functools.partial(gather_stages_x, "z", "y"))
        return [make(w, full, local.at[i], sems[2 * i], sems[2 * i + 1]) for i, (make, w, full) in enumerate(zip(makers, ins, outs, strict=True))]

    @staticmethod
    def whole_matrices(fulls):
        return [f.reshape(-1, f.shape[-1]) for f in fulls]


def gather_stages_chunk(first, second, w, full, local, send, recv, start, size, to=None):
    wires = Wires(send, recv)
    to = start if to is None else to
    source = w.at[:, pl.ds(start, size)]
    cols, left, right = pl.ds(to, size), pl.ds(to, size // 2), pl.ds(to + size // 2, size // 2)

    def part(p, c):
        return full.at[p["y"], p["z"], p["c"], :, c]

    def row(p, c):
        return part({**p, first: slice(None)}, c)

    def s0():
        me = here()
        for j in (1, 3, 2):
            wires.go(j - 1, source, part(me, cols), moved(me, first, j))
        pltpu.make_async_copy(source, part(me, cols), local).start()

    def s1():
        me = here()
        pltpu.make_async_copy(source, part(me, cols), local).wait()
        for j in (1, 3, 2):
            wires.wait(j - 1, part(moved(me, first, 4 - j), cols), me)
        wires.go(3, row(me, cols), row(me, cols), moved(me, second, 1))
        wires.go(4, row(me, cols), row(me, cols), moved(me, second, 3))

    def s2():
        me = here()
        before, after = moved(me, second, 3), moved(me, second, 1)
        wires.wait(3, row(before, cols), me)
        wires.go(5, row(before, left), row(before, left), after)
        wires.wait(4, row(after, cols), me)
        wires.go(6, row(after, right), row(after, right), before)

    def every(c):
        return full.at[:, :, c, :, cols]

    def s3():
        me = here()
        far, mate = moved(me, second, 2), moved(me, "c", 1)
        wires.wait(5, row(far, left), me)
        wires.wait(6, row(far, right), me)
        wires.go(7, every(me["c"]), every(me["c"]), mate)

    def s4():
        me = here()
        wires.wait(7, every(moved(me, "c", 1)["c"]), me)

    def s5():
        me = here()
        for j in range(3):
            wires.sent(j, source, me)
        for i, c in ((3, cols), (4, cols), (5, left), (6, right)):
            wires.sent(i, row(me, c), me)
        wires.sent(7, every(me["c"]), me)

    return [s0, s1, s2, s3, s4, s5]


SUM_PEERS = (("c", 1), *((axis, step) for axis in "xyz" for step in (1, 2, 3)))
SUM_SEMS = 20
SUM_ORDERS = ("xyz", "yzx", "zxy")


def sum_scratch(rows, columns):
    w = columns // 4
    vm = lambda *shape: pltpu.VMEM((*shape, rows, w), BF16)
    wide = lambda *shape: pltpu.VMEM((*shape, rows, w), F32)
    return [
        *[pltpu.VMEM((4, 4, rows, columns), BF16)] * 2,
        vm(2, 8), vm(2, 8), vm(2, 16), vm(2, 16), wide(16),
        vm(2, 2), vm(2, 2), vm(2, 4), vm(2, 4), wide(4),
        vm(3), vm(3), vm(4),
        pltpu.SemaphoreType.DMA((12,)), pltpu.SemaphoreType.DMA((SUM_SEMS,)), pltpu.SemaphoreType.DMA((SUM_SEMS,)),
    ]


SUM_REFS = 18


def sum_stages(order, term, there, out, refs):
    own, mates, o1, i1, o2, i2, k1, o3, i3, o4, i4, k2, o5, i5, ob, local, send, recv = refs
    wires = Wires(send, recv)
    A, B, D = order
    w = out.shape[-1] // 4

    def lane(q):
        return pl.ds(pl.multiple_of(q * w, 128), w)

    def chip(p):
        at = p["y"], p["z"], slice(None), lane(p["x"])
        return own[at].astype(F32) + mates[at].astype(F32)

    QUARTERS = (2, 1, 3, 0)

    def quarter(ref, me, k, core=None):
        n = lax.rem(me[A] + QUARTERS[k], 4)
        y, z, x = (n if A == axis else slice(None) for axis in "yzx")
        cols = lane(n) if A == "x" else slice(None)
        return ref.at[y, z, :, cols] if core is None else ref.at[y, z, core, :, cols]

    def fetch(me, k):
        return pltpu.make_async_copy(quarter(term, me, k, me["c"]), quarter(own, me, k), local.at[k])

    def fetch_mates(me, k):
        return pltpu.make_async_copy(quarter(there, me, k), quarter(mates, me, k), local.at[8 + k])

    def r0():
        me = here()
        mate = moved(me, "c", 1)
        for k in range(4):
            if there is None:
                wires.go(k, quarter(term, me, k, mate["c"]), quarter(mates, me, k), mate)
            else:
                fetch_mates(me, k).start()
            fetch(me, k).start()

    def have(me, k):
        fetch(me, k).wait()
        if there is None:
            wires.wait(k, quarter(mates, me, k), me)
        else:
            fetch_mates(me, k).wait()

    def r1():
        me = here()
        have(me, 0)
        far = lax.rem(me[A] + 2, 4)
        for turn, step in ((0, 1), (1, 3)):

            @pl.loop(0, 8)
            def _(i):
                b, d = lax.div(i, 4), lax.rem(i, 4)
                o1[turn, i] = chip({A: far, B: 2 * turn + b, D: d}).astype(BF16)

            wires.go(4 + turn, o1.at[turn], i1.at[turn], moved(me, A, step))
        for turn, step in ((0, 1), (1, 3)):
            to = moved(me, A, step)
            have(me, 1 + turn)

            @pl.loop(0, 8)
            def _(i):
                b, d = lax.div(i, 4), lax.rem(i, 4)
                o2[turn, 8 * (1 - turn) + i] = chip({A: to[A], B: 2 * (1 - turn) + b, D: d}).astype(BF16)

            rest = pl.ds(8 * (1 - turn), 8)
            wires.go(18 + turn, o2.at[turn, rest], i2.at[turn, rest], to)

    def r2():
        me = here()
        for turn, step in ((0, 1), (1, 3)):
            wires.wait(4 + turn, i1.at[turn], me)
            to = moved(me, A, step)

            @pl.loop(0, 8)
            def _(i):
                b, d = lax.div(i, 4), lax.rem(i, 4)
                o2[turn, 8 * turn + i] = (chip({A: to[A], B: 2 * turn + b, D: d}) + i1[turn, i].astype(F32)).astype(BF16)

            added = pl.ds(8 * turn, 8)
            wires.go(6 + turn, o2.at[turn, added], i2.at[turn, added], to)

    def r3():
        me = here()
        have(me, 3)
        for turn in (0, 1):
            wires.wait(18 + turn, i2.at[turn, pl.ds(8 * (1 - turn), 8)], me)
            wires.wait(6 + turn, i2.at[turn, pl.ds(8 * turn, 8)], me)

        @pl.loop(0, 16)
        def _(i):
            k1[i] = chip({A: me[A], B: lax.div(i, 4), D: lax.rem(i, 4)}) + i2[0, i].astype(F32) + i2[1, i].astype(F32)

        far = lax.rem(me[B] + 2, 4)
        for turn, step in ((0, 1), (1, 3)):
            for d in range(2):
                o3[turn, d] = k1[far * 4 + 2 * turn + d].astype(BF16)
            wires.go(8 + turn, o3.at[turn], i3.at[turn], moved(me, B, step))

    def r4():
        me = here()
        for turn, step in ((0, 1), (1, 3)):
            wires.wait(8 + turn, i3.at[turn], me)
            to = moved(me, B, step)
            for d in range(2):
                o4[turn, 2 * turn + d] = (k1[to[B] * 4 + 2 * turn + d] + i3[turn, d].astype(F32)).astype(BF16)
                o4[turn, 2 * (1 - turn) + d] = k1[to[B] * 4 + 2 * (1 - turn) + d].astype(BF16)
            wires.go(10 + turn, o4.at[turn], i4.at[turn], to)

    def r5():
        me = here()
        for turn in (0, 1):
            wires.wait(10 + turn, i4.at[turn], me)
        for d in range(4):
            k2[d] = k1[me[B] * 4 + d] + i4[0, d].astype(F32) + i4[1, d].astype(F32)
        for j in (1, 2, 3):
            to = moved(me, D, j)
            o5[j - 1] = k2[to[D]].astype(BF16)
            wires.go(11 + j, o5.at[j - 1], i5.at[j - 1], to)

    def r6():
        me = here()
        total = k2[me[D]]
        for j in (1, 2, 3):
            wires.wait(11 + j, i5.at[j - 1], me)
            total = total + i5[j - 1].astype(F32)
        ob[me["x"]] = total.astype(BF16)
        for j in (1, 2, 3):
            wires.go(14 + j, ob.at[me["x"]], ob.at[me["x"]], moved(me, "x", j))

    def put(q):
        return pltpu.make_async_copy(ob.at[q], out.at[:, pl.ds(q * w, w)], local.at[4 + q])

    def r7():
        me = here()
        for j in (1, 2, 3):
            wires.wait(14 + j, ob.at[moved(me, "x", 4 - j)["x"]], me)
        for q in range(4):
            put(q).start()
        for k in range(4):
            if there is None:
                wires.sent(k, quarter(mates, me, k), me)
        for turn in (0, 1):
            wires.sent(4 + turn, o1.at[turn], me)
            wires.sent(6 + turn, o2.at[turn, pl.ds(8 * turn, 8)], me)
            wires.sent(18 + turn, o2.at[turn, pl.ds(8 * (1 - turn), 8)], me)
            wires.sent(8 + turn, o3.at[turn], me)
            wires.sent(10 + turn, o4.at[turn], me)
        for j in (1, 2, 3):
            wires.sent(11 + j, o5.at[j - 1], me)
            wires.sent(14 + j, ob.at[me["x"]], me)
        for q in range(4):
            put(q).wait()

    return [r0, r1, r2, r3, r4, r5, r6, r7]


def cut(term):
    return term.reshape(4, 4, 2, term.shape[0] // 32, term.shape[1])


class Mates(Exchange):
    peers = (("c", 1),)

    def __init__(self, terms):
        self.operands = [cut(t) for t in terms]
        self.in_specs = [ANY] * len(terms)
        self.out_shape = [jax.ShapeDtypeStruct((4, 4, *t.shape[3:]), BF16) for t in self.operands]
        self.out_specs = [ANY] * len(terms)
        self.scratch = [pltpu.SemaphoreType.DMA((len(terms),))] * 2

    def plan(self, ins, outs, scratch):
        wires = Wires(*scratch)

        def begin():
            mate = moved(here(), "c", 1)
            for n, (term, out) in enumerate(zip(ins, outs, strict=True)):
                wires.go(n, term.at[:, :, mate["c"]], out, mate)

        def end():
            me = here()
            for n, out in enumerate(outs):
                wires.wait(n, out, me)
                wires.sent(n, out, me)

        return [[begin, end]]


MATES_MARKS = {0: [(0, 0)], "end": [(0, 1)]}


class Sum(Exchange):
    peers = SUM_PEERS

    def __init__(self, terms, mates=()):
        self.n = len(terms)
        terms = [cut(t) for t in terms]
        self.operands = [*terms, *mates]
        self.in_specs = [ANY] * len(self.operands)
        self.out_shape = [jax.ShapeDtypeStruct(t.shape[3:], BF16) for t in terms]
        self.out_specs = [ANY] * self.n
        self.scratch = [s for t in terms for s in sum_scratch(*t.shape[3:])]

    def plan(self, ins, outs, scratch):
        theres = list(ins[self.n :]) or [None] * self.n
        return [sum_stages(SUM_ORDERS[i], ins[i], theres[i], outs[i], scratch[SUM_REFS * i : SUM_REFS * (i + 1)]) for i in range(self.n)]


def all_of(*numbers):
    return [(which, number) for number in numbers for which in range(3)]


SUM_LONG_MARKS = {0: all_of(0), 1: all_of(1), 3: all_of(2), 6: all_of(3), 7: all_of(4), 8: all_of(5), 9: all_of(6), "end": all_of(7)}
SUM_SHORT_MARKS = {0: all_of(0, 1), 3: all_of(2), 6: all_of(3), 7: all_of(4), "end": all_of(5, 6, 7)}


def dot(a, b, dims=((1,), (0,))):
    return lax.dot_general(a, b, (dims, ((), ())), preferred_element_type=F32)


def scale_of(wide):
    return lax.rsqrt(jnp.mean(wide * wide, -1, keepdims=True) + 1e-6)


def norm_into(h, a, at, chunk=512):
    @pl.loop(0, h.shape[0], step=chunk)
    def _(m):
        rows = pl.ds(m, chunk)
        wide = h[rows, :].astype(F32)
        value = (wide * scale_of(wide)).astype(BF16)
        if a is not None:
            a[rows, :] = value
        if at is not None:
            at[:, rows] = value.T


def whole(shape):
    return pl.BlockSpec(shape, lambda i: (0,) * len(shape), pipeline_mode=pl.Buffered(1))


TILE, CHUNK, CHUNK_FRESH, CHUNK_HIDDEN = 256, 512, 1024, 256


def call(kernel, grid, operands, in_specs, out_shape, out_specs, scratch, name, exchange=None, marks=None, collective_id=None):
    counts = [len(operands), len(out_shape), len(scratch)]
    extra = [exchange.operands, exchange.out_shape, exchange.scratch] if exchange else [[], [], []]
    n_extra = [len(e) for e in extra]

    def body(*refs):
        refs, mine, theirs = list(refs), [], []
        for n, k in zip(counts, n_extra, strict=True):
            mine += refs[:n]
            theirs.append(refs[n : n + k])
            refs = refs[n + k :]
        i = pl.program_id(0)
        if exchange:
            plan = exchange.plan(*theirs)
            exchange.grid_step(plan, marks, i)
        kernel(*mine)
        if exchange:

            @pl.when(i == grid - 1)
            def _():
                exchange.finish(plan, marks)

    params = dict(collective_id=collective_id, has_side_effects=True) if exchange else {}
    out = pl.pallas_call(
        body,
        grid=(grid,),
        out_shape=list(out_shape) + (exchange.out_shape if exchange else []),
        in_specs=list(in_specs) + (exchange.in_specs if exchange else []),
        out_specs=list(out_specs) + (exchange.out_specs if exchange else []),
        scratch_shapes=list(scratch) + (exchange.scratch if exchange else []),
        compiler_params=pltpu.CompilerParams(vmem_limit_bytes=LIMIT, **params),
        name=name,
    )(*operands, *(exchange.operands if exchange else []))
    return out[: counts[1]], out[counts[1] :]


PIECES = ((0, 256, 0), (256, 256, 1), (512, 512, 2), (1024, 512, 4), (1536, 512, 6), (2048, 512, 8))
PIECES_AT = ((-4, -1, 0, 99), (-3, -2, -1, 0, 1, 99), (-2, -1, 0, 1, 2, 99), (0, 1, 2, 3, 4, 99), (2, 3, 4, 5, 6, 99), (4, 5, 6, 7, 8, 99))
DOWN_AT = (-4, -2, -1, 0, 1, 5, 7, 9)
NEXT_DOWN_AT = (1, 2, 3, 4, 6, 10, 12, 99)
NEXT_AT = (5, 6, 7, 10, 11, 99)
EARLY = 1024


def forward(h, weights, collective_id):
    tokens, d = h.shape
    ff = weights[0].shape[2]
    tiles, outs = ff // TILE, d // TILE
    steps = tiles + outs
    pieces = len(PIECES)
    now = [jax.ShapeDtypeStruct(w.shape[1:], BF16) for w in weights]
    later = [jax.ShapeDtypeStruct((w.shape[1], EARLY), BF16) for w in weights[:2]] + now[2:]
    next_layer = Gather(later)

    def kernel(h_ref, wg_ref, wu_ref, wd_ref, y_ref, g_ref, u_ref, at_ref, fg, fu, fd, hg, hu, hd, a, act, vg, vu, vd, local, csend, crecv, dsend, drecv, *scratch):
        i = pl.program_id(0)
        ng, nu, nd = wg_ref.at[0], wu_ref.at[0], wd_ref.at[0]
        lg, lu, ld = wg_ref.at[1, :, pl.ds(0, EARLY)], wu_ref.at[1, :, pl.ds(0, EARLY)], wd_ref.at[1]
        todo = {}

        def plan(at, stages):
            for k, stage in zip(at, stages):
                todo.setdefault(min(k, steps), []).append(stage)

        def keep(n, src, dst):
            return pltpu.make_async_copy(src, dst, local.at[2 * pieces + 1 + n])

        matrices = ((("z", "y"), ng, vg), (("y", "z"), nu, vu))
        for k in reversed(range(pieces)):
            start, size, _ = PIECES[k]
            for m, (order, w, full) in enumerate(matrices):
                n = m * pieces + k
                if k == 0:
                    plan(PIECES_AT[k], gather_stages_direct(w, full, local.at[n], dsend.at[m], drecv.at[m], start, size))
                else:
                    plan(PIECES_AT[k], gather_stages_chunk(*order, w, full, local.at[n], csend.at[n], crecv.at[n], start, size))
        plan(DOWN_AT, gather_stages_x("z", "y", nd, vd, local.at[2 * pieces], dsend.at[2], drecv.at[2]))
        plan((tiles, tiles, tiles, 99, 99, 99), [keep(0, vg, fg).start, keep(1, vu, fu).start, keep(2, vd, fd).start, keep(0, vg, fg).wait, keep(1, vu, fu).wait, keep(2, vd, fd).wait])
        after = next_layer.plan((lg, lu, ld), (hg, hu, hd), scratch)
        for which, at in enumerate((NEXT_AT, NEXT_AT, NEXT_DOWN_AT)):
            plan(at, after[which])

        @pl.when(i == 0)
        def _():
            greet(PLANE_PEERS)
            for t in sorted(todo):
                if t < 0:
                    for f in todo[t]:
                        f()
                if t == -3:
                    norm_into(h_ref, a, at_ref)

        for at in range(steps):
            if at in todo:

                @pl.when(i == at)
                def _():
                    for f in todo[at]:
                        f()

        @pl.when(i < tiles)
        def _():
            cols = pl.ds(pl.multiple_of(i * TILE, TILE), TILE)
            wg = vg[:, :, :, :, cols].reshape(d, TILE)
            wu = vu[:, :, :, :, cols].reshape(d, TILE)

            @pl.loop(0, tokens, step=CHUNK, unroll=True)
            def _(m):
                rows = pl.ds(m, CHUNK)
                g = dot(a[rows, :], wg)
                u = dot(a[rows, :], wu)
                g_ref[rows, :] = g
                u_ref[rows, :] = u
                act[i, rows, :] = (g * jax.nn.sigmoid(g) * u).astype(BF16)

        @pl.when(i >= tiles)
        def _():
            cols = pl.ds(pl.multiple_of((i - tiles) * TILE, TILE), TILE)

            @pl.loop(0, tokens, step=CHUNK, unroll=True)
            def _(m):
                rows = pl.ds(m, CHUNK)
                total = sum(dot(act[k, rows, :], vd[:, :, :, :, cols].reshape(ff, TILE)[k * TILE : (k + 1) * TILE, :]) for k in range(tiles))
                y_ref[rows, :] = h_ref[rows, cols] + total.astype(BF16)

        @pl.when(i == steps - 1)
        def _():
            for f in todo[steps]:
                f()

    tile = pl.BlockSpec((tokens, TILE), lambda i: (0, jnp.minimum(i, tiles - 1)))
    full_types = [jax.ShapeDtypeStruct(blocks_of(w), BF16) for w in (*now, *later)]
    dma = pltpu.SemaphoreType.DMA
    out = pl.pallas_call(
        kernel,
        grid=(steps,),
        out_shape=[
            jax.ShapeDtypeStruct(h.shape, BF16),
            jax.ShapeDtypeStruct((tokens, ff), F32),
            jax.ShapeDtypeStruct((tokens, ff), F32),
            jax.ShapeDtypeStruct((d, tokens), BF16),
            *full_types,
        ],
        in_specs=[whole(h.shape)] + [whole(w.shape) for w in weights],
        out_specs=[pl.BlockSpec((tokens, TILE), lambda i: (0, jnp.maximum(i - tiles, 0))), tile, tile, whole((d, tokens))] + [ANY] * 6,
        scratch_shapes=[
            pltpu.VMEM(h.shape, BF16),
            pltpu.VMEM((tiles, tokens, TILE), BF16),
            *(pltpu.VMEM(t.shape, BF16) for t in full_types[:3]),
            dma((2 * pieces + 4,)),
            dma((2 * pieces, 8)),
            dma((2 * pieces, 8)),
            dma((3, 16)),
            dma((3, 16)),
            *next_layer.scratch,
        ],
        compiler_params=pltpu.CompilerParams(vmem_limit_bytes=LIMIT, collective_id=collective_id, has_side_effects=True),
        name="forward",
    )(h, *weights)
    return out[:4], [f.reshape(-1, f.shape[-1]) for f in out[4:]]


def hidden_grads(g, u, by_act):
    sig = jax.nn.sigmoid(g)
    silu = g * sig
    by_act = by_act.astype(BF16).astype(F32)
    return (silu * u).astype(BF16), (by_act * u * (sig * (1 + g * (1 - sig)))).astype(BF16), (by_act * silu).astype(BF16)


def backward_fresh(h, by_y, early, weights, wd, collective_id):
    tokens, d = h.shape
    ff = wd.shape[0]
    steps, first = ff // TILE, EARLY // TILE
    late = ff - EARLY

    def kernel(h_ref, ga, ua, wg_ref, wu_ref, by_ref, wd_ref, dg_ref, du_ref, dwg_ref, dwu_ref, dwd_ref, hg, hu, a, at, act, tg, tu, vg, vu, local, send, recv):
        i = pl.program_id(0)
        lists = [
            gather_stages_chunk(*order, w.at[1], full, local.at[n], send.at[n], recv.at[n], EARLY, late, 0)
            for n, (order, w, full) in enumerate(((("z", "y"), wg_ref, vg), (("y", "z"), wu_ref, vu)))
        ]
        keep = [pltpu.make_async_copy(v, o, local.at[2 + n]) for n, (v, o) in enumerate(((vg, hg), (vu, hu)))]

        for at_step in range(first + 1):

            @pl.when(i == at_step)
            def _():
                if at_step == 0:
                    greet(Gather.peers)
                for stages in lists:
                    stages[at_step]()
                if at_step == 0:
                    norm_into(h_ref, a, at)
                if at_step == first:
                    for k in keep:
                        k.start()

        @pl.when(i < first)
        def _():
            cols = pl.ds(pl.multiple_of(i * TILE, TILE), TILE)
            tg[...] = ga[:, cols]
            tu[...] = ua[:, cols]

        @pl.when(i >= first)
        def _():
            cols = pl.ds(pl.multiple_of((i - first) * TILE, TILE), TILE)
            tg[...] = vg[:, :, :, :, cols].reshape(d, TILE)
            tu[...] = vu[:, :, :, :, cols].reshape(d, TILE)

        @pl.loop(0, tokens, step=CHUNK_FRESH, unroll=True)
        def _(m):
            rows = pl.ds(m, CHUNK_FRESH)
            g, u = dot(a[rows, :], tg[...]), dot(a[rows, :], tu[...])
            by_act = dot(by_ref[rows, :], wd_ref[...], ((1,), (1,)))
            act[rows, :], dg_ref[rows, :], du_ref[rows, :] = hidden_grads(g, u, by_act)

        dwd_ref[...] = dot(act[...], by_ref[...], ((0,), (0,))).astype(BF16)
        dwg_ref[...] = dot(at[...], dg_ref[...]).astype(BF16)
        dwu_ref[...] = dot(at[...], du_ref[...]).astype(BF16)

        @pl.when(i == steps - 1)
        def _():
            for stages in lists:
                stages[5]()
            for k in keep:
                k.wait()

    across = pl.BlockSpec((d, TILE), lambda i: (0, i))
    down = pl.BlockSpec((TILE, d), lambda i: (i, 0))
    tile = pl.BlockSpec((tokens, TILE), lambda i: (0, i))
    part = (4, 4, 2, d // 32, late)
    dma = pltpu.SemaphoreType.DMA
    out = pl.pallas_call(
        kernel,
        grid=(steps,),
        out_shape=[jax.ShapeDtypeStruct((tokens, ff), BF16)] * 2
        + [jax.ShapeDtypeStruct((d, ff), BF16)] * 2
        + [jax.ShapeDtypeStruct((ff, d), BF16)]
        + [jax.ShapeDtypeStruct(part, BF16)] * 2,
        in_specs=[whole((tokens, d)), *[whole((d, EARLY))] * 2, *[whole(w.shape) for w in weights[:2]], whole((tokens, d)), down],
        out_specs=[tile, tile, across, across, down, ANY, ANY],
        scratch_shapes=[
            pltpu.VMEM((tokens, d), BF16),
            pltpu.VMEM((d, tokens), BF16),
            pltpu.VMEM((tokens, TILE), BF16),
            *[pltpu.VMEM((d, TILE), BF16)] * 2,
            *[pltpu.VMEM(part, BF16)] * 2,
            dma((4,)),
            dma((2, 8)),
            dma((2, 8)),
        ],
        compiler_params=pltpu.CompilerParams(vmem_limit_bytes=LIMIT, collective_id=collective_id, has_side_effects=True),
        name="backward_fresh",
    )(h, *early, *weights[:2], by_y, wd)
    return out[:2], out[2:5], [f.reshape(d, late) for f in out[5:]]


def backward_hidden(by_y, wd, saved, **beside):
    tokens, d = by_y.shape
    ff = wd.shape[0]
    steps = ff // TILE

    def kernel(at, g_ref, u_ref, by_ref, wd_ref, dg_ref, du_ref, dwg_ref, dwu_ref, dwd_ref, act):
        @pl.loop(0, tokens, step=CHUNK_HIDDEN, unroll=True)
        def _(m):
            rows = pl.ds(m, CHUNK_HIDDEN)
            by_act = dot(by_ref[rows, :], wd_ref[...], ((1,), (1,)))
            act[rows, :], dg_ref[rows, :], du_ref[rows, :] = hidden_grads(g_ref[rows, :], u_ref[rows, :], by_act)

        dwd_ref[...] = dot(act[...], by_ref[...], ((0,), (0,))).astype(BF16)
        dwg_ref[...] = dot(at[...], dg_ref[...]).astype(BF16)
        dwu_ref[...] = dot(at[...], du_ref[...]).astype(BF16)

    across = pl.BlockSpec((d, TILE), lambda i: (0, i))
    down = pl.BlockSpec((TILE, d), lambda i: (i, 0))
    tile = pl.BlockSpec((tokens, TILE), lambda i: (0, i))
    return call(
        kernel,
        steps,
        (*saved, by_y, wd),
        [whole((d, tokens)), tile, tile, whole((tokens, d)), down],
        [jax.ShapeDtypeStruct((tokens, ff), BF16)] * 2 + [jax.ShapeDtypeStruct((d, ff), BF16)] * 2 + [jax.ShapeDtypeStruct((ff, d), BF16)],
        [tile, tile, across, across, down],
        [pltpu.VMEM((tokens, TILE), BF16)],
        "backward_hidden",
        **beside,
    )


def backward_input(dg, du, wgs, wus, h, by_y, **beside):
    tokens, d = h.shape
    ff = dg.shape[1]
    chunk = 256

    n = len(wgs)

    def kernel(dg_ref, du_ref, *refs):
        parts, (h_ref, by_ref, out_ref) = refs[: 2 * n], refs[2 * n :]
        by_a, start = 0, 0
        for wg_ref, wu_ref in zip(parts[:n], parts[n:], strict=True):
            cols = pl.ds(start, wg_ref.shape[1])
            start += wg_ref.shape[1]
            by_a = by_a + dot(dg_ref[:, cols], wg_ref[...], ((1,), (1,))) + dot(du_ref[:, cols], wu_ref[...], ((1,), (1,)))
        by_a = by_a.astype(BF16).astype(F32)
        wide = h_ref[...].astype(F32)
        scale = scale_of(wide)
        back = jnp.sum(by_a * wide, -1, keepdims=True) * (scale * scale * scale) * (1 / d)
        out_ref[...] = by_ref[...] + (by_a * scale - wide * back).astype(BF16)

    rows = lambda n: pl.BlockSpec((chunk, n), lambda i: (i, 0))
    return call(
        kernel,
        tokens // chunk,
        (dg, du, *wgs, *wus, h, by_y),
        [rows(ff), rows(ff), *(whole(w.shape) for w in (*wgs, *wus)), rows(d), rows(d)],
        [jax.ShapeDtypeStruct(h.shape, BF16)],
        [rows(d)],
        [],
        "backward_input",
        **beside,
    )


def results(by_x, layers):
    n, tokens = len(layers[0]), by_x.shape[0]
    steps = 4

    def kernel(x_ref, *refs):
        out_ref, outs = refs[len(layers) * n], refs[len(layers) * n + 1 :]
        out_ref[...] = x_ref[...]

        @pl.when(pl.program_id(0) == 0)
        def _():
            for k in range(n):
                for layer in range(len(layers)):
                    outs[k][layer] = refs[layer * n + k][...]

    rows = pl.BlockSpec((tokens // steps, by_x.shape[1]), lambda i: (i, 0))
    shapes = [(len(layers), *t.shape) for t in layers[0]]
    return pl.pallas_call(
        kernel,
        grid=(steps,),
        out_shape=[jax.ShapeDtypeStruct(by_x.shape, BF16)] + [jax.ShapeDtypeStruct(shape, BF16) for shape in shapes],
        in_specs=[rows] + [whole(t.shape) for layer in layers for t in layer],
        out_specs=[rows] + [whole(shape) for shape in shapes],
        name="results",
    )(by_x, *(t for layer in layers for t in layer))


def solution(mesh):
    def step(x, dy, *weights):
        x, dy = x[0], dy[0]
        (h1, g0, u0, at0), (wg0, wu0, wd0, wg1, wu1, wd1) = forward(x, weights, 1)
        (dg1, du1), terms1, (wg1_rest, wu1_rest) = backward_fresh(h1, dy, (wg1, wu1), weights, wd1, 2)
        (by_h1,), mates1 = backward_input(dg1, du1, (wg1, wg1_rest), (wu1, wu1_rest), h1, dy, exchange=Mates(terms1), marks=MATES_MARKS, collective_id=3)
        (dg0, du0, *terms0), sums1 = backward_hidden(by_h1, wd0, (at0, g0, u0), exchange=Sum(terms1, mates1), marks=SUM_LONG_MARKS, collective_id=4)
        (by_x,), sums0 = backward_input(dg0, du0, (wg0,), (wu0,), x, by_h1, exchange=Sum(terms0), marks=SUM_SHORT_MARKS, collective_id=5)
        by_x, *by_weights = results(by_x, [sums0, sums1])
        return (by_x[None], *by_weights)

    states, shard = P(("rep", "r", "s"), None, None), P(None, "s", None)
    return jax.shard_map(
        step,
        mesh=mesh,
        in_specs=(states, states) + (shard,) * 3,
        out_specs=(states,) + (P("rep", "s", None),) * 3,
        check_vma=False,
    )
```
